128 devices in a mesh: dp: 128 (over z, y, x, core).
Axes of the slice: x: 4, y: 4, z: 4, core: 2. Of those that a mesh axis runs over, the one named last changes fastest.
Arguments:
- user_x: float32 [16384, 256], P('dp')
- item_x: float32 [16384, 256], P('dp')
- item_id: int32 [16384], P('dp')
- log_q: float32 [16384], P('dp')
- user_w1: float32 [256, 384], replicated
- user_w2: float32 [384, 384], replicated
- user_w3: float32 [384, 128], replicated
- item_w1: float32 [256, 384], replicated
- item_w2: float32 [384, 384], replicated
- item_w3: float32 [384, 128], replicated
Outputs:
- output 1: float32 [], replicated
- output 2: float32 [256, 384], replicated
- output 3: float32 [384, 384], replicated
- output 4: float32 [384, 128], replicated
- output 5: float32 [256, 384], replicated
- output 6: float32 [384, 384], replicated
- output 7: float32 [384, 128], replicated
All inputs are finite; a program needn't handle non-finite values.
Results may differ from the reference program's by a relative error of at most 0.0021784.
Values are sent between devices in bfloat16 or wider.
A program may use at most 1 GiB of HBM per device.

```python
import jax
import jax.numpy as jnp
from jax import lax

ROWS_DEV = 128
GROUP_SIZE = 128
IN_WIDTH = 256
HIDDEN_A = 384
HIDDEN_B = 384
EMBED_DIM = 128

BATCH = ROWS_DEV * GROUP_SIZE
ID_RANGE = max(BATCH // 64, 2)
TEMPERATURE = 0.05
INV_TEMP = 1.0 / TEMPERATURE
NORM_EPS = 1e-6


def id_features(key, item_id):
    def one_row(one_id):
        return jax.random.normal(jax.random.fold_in(key, one_id), (IN_WIDTH,), jnp.float32)
    return jax.vmap(one_row)(item_id)


def setup_inputs(seed: int = 0) -> dict:
    keys = jax.random.split(jax.random.key(seed), 12)
    shapes = ((IN_WIDTH, HIDDEN_A), (HIDDEN_A, HIDDEN_B), (HIDDEN_B, EMBED_DIM))
    gains = (2.0, 2.0, 1.0)
    user_ws = []
    item_ws = []
    for layer in range(3):
        scale = (gains[layer] / shapes[layer][0]) ** 0.5
        base = jax.random.normal(keys[layer], shapes[layer], jnp.float32)
        other = jax.random.normal(keys[layer + 3], shapes[layer], jnp.float32)
        user_ws.append(base * scale)
        item_ws.append((0.95 * base + 0.31 * other) * scale)
    item_id = jax.random.randint(keys[6], (BATCH,), 0, ID_RANGE, dtype=jnp.int32)
    item_x = 0.97 * id_features(keys[7], item_id) + 0.243 * jax.random.normal(keys[8], (BATCH, IN_WIDTH), jnp.float32)
    user_x = 0.95 * item_x + 0.31 * jax.random.normal(keys[9], (BATCH, IN_WIDTH), jnp.float32)
    log_q = jax.random.uniform(keys[10], (BATCH,), jnp.float32, -12.0, -6.0)
    return {'user_x': user_x, 'item_x': item_x, 'item_id': item_id, 'log_q': log_q,
            'user_w1': user_ws[0], 'user_w2': user_ws[1], 'user_w3': user_ws[2],
            'item_w1': item_ws[0], 'item_w2': item_ws[1], 'item_w3': item_ws[2]}


def tower_forward(inputs, w_one, w_two, w_three):
    x_half = inputs.astype(jnp.bfloat16)
    pre_one = jnp.dot(x_half, w_one.astype(jnp.bfloat16), preferred_element_type=jnp.float32)
    act_one = jnp.maximum(pre_one, 0.0).astype(jnp.bfloat16)
    pre_two = jnp.dot(act_one, w_two.astype(jnp.bfloat16), preferred_element_type=jnp.float32)
    act_two = jnp.maximum(pre_two, 0.0).astype(jnp.bfloat16)
    raw_out = jnp.dot(act_two, w_three.astype(jnp.bfloat16), preferred_element_type=jnp.float32)
    inv_norm = lax.rsqrt(jnp.sum(raw_out * raw_out, axis=1, keepdims=True) + NORM_EPS)
    return (x_half, pre_one, act_one, pre_two, act_two, raw_out * inv_norm, inv_norm)


def tower_grads(inputs, w_one, w_two, w_three, grad_unit):
    x_half, pre_one, act_one, pre_two, act_two, unit_out, inv_norm = tower_forward(inputs, w_one, w_two, w_three)
    grad_raw = inv_norm * (grad_unit - unit_out * jnp.sum(unit_out * grad_unit, axis=1, keepdims=True))
    grad_raw_h = grad_raw.astype(jnp.bfloat16)
    grad_three = jnp.dot(act_two.T, grad_raw_h, preferred_element_type=jnp.float32)
    grad_act_two = jnp.dot(grad_raw_h, w_three.astype(jnp.bfloat16).T, preferred_element_type=jnp.float32)
    grad_pre_two = jnp.where(pre_two > 0.0, grad_act_two, 0.0).astype(jnp.bfloat16)
    grad_two = jnp.dot(act_one.T, grad_pre_two, preferred_element_type=jnp.float32)
    grad_act_one = jnp.dot(grad_pre_two, w_two.astype(jnp.bfloat16).T, preferred_element_type=jnp.float32)
    grad_pre_one = jnp.where(pre_one > 0.0, grad_act_one, 0.0).astype(jnp.bfloat16)
    grad_one = jnp.dot(x_half.T, grad_pre_one, preferred_element_type=jnp.float32)
    return (grad_one, grad_two, grad_three)


def accumulate_grads(x_shards, grad_shards, w_one, w_two, w_three):
    def grad_step(carry, shard):
        step_grads = tower_grads(shard[0], w_one, w_two, w_three, shard[1])
        return tuple(total + part for total, part in zip(carry, step_grads)), None
    zeros = (jnp.zeros(w_one.shape, jnp.float32), jnp.zeros(w_two.shape, jnp.float32), jnp.zeros(w_three.shape, jnp.float32))
    return lax.scan(grad_step, zeros, (x_shards, grad_shards))[0]


def reference(user_x, item_x, item_id, log_q, user_w1, user_w2, user_w3, item_w1, item_w2, item_w3):
    user_shards = user_x.reshape(GROUP_SIZE, ROWS_DEV, IN_WIDTH)
    item_shards = item_x.reshape(GROUP_SIZE, ROWS_DEV, IN_WIDTH)
    user_half = lax.map(lambda rows_in: tower_forward(rows_in, user_w1, user_w2, user_w3)[5], user_shards).astype(jnp.bfloat16)
    item_half = lax.map(lambda rows_in: tower_forward(rows_in, item_w1, item_w2, item_w3)[5], item_shards).astype(jnp.bfloat16)
    item_all = item_half.reshape(BATCH, EMBED_DIM)
    cand_pos = jnp.arange(BATCH)

    def query_step(grad_item_sum, shard):
        user_rows, item_rows, id_rows, logq_rows, shard_index = shard
        query_pos = shard_index * ROWS_DEV + jnp.arange(ROWS_DEV)
        raw = jnp.dot(user_rows, item_all.T, preferred_element_type=jnp.float32) * INV_TEMP - log_q[None, :]
        is_self = query_pos[:, None] == cand_pos[None, :]
        dropped = jnp.logical_and(id_rows[:, None] == item_id[None, :], jnp.logical_not(is_self))
        scores = jnp.where(dropped, -jnp.inf, raw)
        row_max = jnp.max(scores, axis=1, keepdims=True)
        exp_scores = jnp.exp(scores - row_max)
        row_total = jnp.sum(exp_scores, axis=1, keepdims=True)
        log_norm = row_max[:, 0] + jnp.log(row_total[:, 0])
        pos_score = jnp.sum(user_rows.astype(jnp.float32) * item_rows.astype(jnp.float32), axis=1) * INV_TEMP - logq_rows
        softmax_rows = exp_scores / row_total
        grad_scores = (jnp.where(is_self, softmax_rows - 1.0, softmax_rows) / BATCH).astype(jnp.bfloat16)
        grad_user = jnp.dot(grad_scores, item_all, preferred_element_type=jnp.float32) * INV_TEMP
        item_part = jnp.dot(grad_scores.T, user_rows, preferred_element_type=jnp.float32) * INV_TEMP
        return grad_item_sum + item_part, (jnp.sum(log_norm - pos_score), grad_user)

    grad_item, step_out = lax.scan(query_step, jnp.zeros((BATCH, EMBED_DIM), jnp.float32),
                                   (user_half, item_half, item_id.reshape(GROUP_SIZE, ROWS_DEV),
                                    log_q.reshape(GROUP_SIZE, ROWS_DEV), jnp.arange(GROUP_SIZE)))
    loss_parts, grad_user = step_out
    user_grads = accumulate_grads(user_shards, grad_user, user_w1, user_w2, user_w3)
    item_grads = accumulate_grads(item_shards, grad_item.reshape(GROUP_SIZE, ROWS_DEV, EMBED_DIM), item_w1, item_w2, item_w3)
    loss = jnp.sum(loss_parts) / BATCH
    return (loss, user_grads[0], user_grads[1], user_grads[2], item_grads[0], item_grads[1], item_grads[2])
```

```python
import functools

import jax
import jax.numpy as jnp
from jax import lax
from jax.experimental import pallas as pl
from jax.experimental.pallas import tpu as pltpu
from jax.sharding import PartitionSpec as P

MESH = pl.DeviceIdType.MESH
F32 = jnp.float32
BF16 = jnp.bfloat16
INV_TEMP = 1.0 / 0.05
NORM_EPS = 1e-6
ROWS = 128
EMB = 128
WIDE = 384
IN_WIDTH = 256
NEG = -3.0e38
GRIDS = {128: (4, 4, 4, 2), 16: (2, 2, 2, 2)}
AZ, AY, AX, AK = range(4)
C00 = (((0,), (0,)), ((), ()))
C11 = (((1,), (1,)), ((), ()))
C10 = (((1,), (0,)), ((), ()))
N_REMOTE = 176


def mm(a, b, dims=C10):
    return lax.dot_general(a, b, dims, preferred_element_type=F32)


def scratch_table(nz, ny, nx, nk):
    n_plane, n_small = nz * ny, nk * nx
    n_tile = n_plane // 2
    n_query = n_small * ROWS
    n_wide = n_plane * ROWS
    longest = max(n_wide, n_query)
    turns = ((nx, ny, nz), (ny, nz, nx), (nz, nx, ny))

    def vm(dtype, *shape):
        return pltpu.VMEM(shape, dtype)

    def two(dtype, *shape):
        return [vm(dtype, *shape) for _ in range(2)]

    def six(shape_of):
        return [[vm(F32, *shape_of(*turn), WIDE) for turn in turns] for _ in range(2)]

    return dict(
        xf=two(F32, ROWS, IN_WIDTH),
        wf=[[vm(F32, IN_WIDTH, WIDE), vm(F32, WIDE, WIDE), vm(F32, WIDE, EMB)] for _ in range(2)],
        wh=[[vm(BF16, IN_WIDTH, WIDE), vm(BF16, WIDE, WIDE), vm(BF16, WIDE, EMB)] for _ in range(2)],
        xt=two(BF16, IN_WIDTH, ROWS),
        h1=two(BF16, ROWS, WIDE),
        h2=two(BF16, ROWS, WIDE),
        h1t=two(BF16, WIDE, ROWS),
        h2t=two(BF16, WIDE, ROWS),
        unit=two(F32, ROWS, EMB),
        inv=two(F32, ROWS, EMB),
        plane=two(BF16, nz, ny, ROWS, EMB),
        small=two(BF16, nk, nx, ROWS, EMB),
        parts=two(F32, n_small, ROWS, EMB),
        from_core=two(F32, nx, ROWS, EMB),
        core_sum=two(F32, nx, ROWS, EMB),
        from_x=two(F32, nx - 1, ROWS, EMB),
        dw=two(F32, nk, 3, ROWS, WIDE),
        from_pair=two(F32, 3, ROWS, WIDE),
        pair_sum=two(F32, 3, ROWS, WIDE),
        ra=six(lambda a, b, c: (a - 1, ROWS // a)),
        sa=six(lambda a, b, c: (ROWS // a,)),
        rb=six(lambda a, b, c: (b - 1, ROWS // a // b)),
        cx=six(lambda a, b, c: (c, ROWS // a // b)),
        res=vm(F32, nk, 2, 3, ROWS, WIDE),
        meta_plane=vm(F32, nz, ny, 8, ROWS),
        meta_small=vm(F32, nk, nx, 8, ROWS),
        lqc_plane=vm(F32, n_plane, ROWS, ROWS),
        idc_plane=vm(jnp.int32, n_plane, ROWS, ROWS),
        lqc_small=vm(F32, n_small, ROWS, ROWS),
        idc_small=vm(jnp.int32, n_small, ROWS, ROWS),
        idr_plane=vm(jnp.int32, 1, n_wide),
        idr_small=vm(jnp.int32, 1, n_query),
        probs=vm(F32, n_tile, 256, n_query),
        tile_max=vm(F32, n_tile, 1, n_query),
        tile_sum=vm(F32, n_tile, 1, n_query),
        factor=vm(F32, n_tile, 1, n_query),
        stats=vm(F32, nk, nx, 2 * n_small, ROWS),
        stat_all=vm(F32, 2 * n_small, ROWS),
        plane_t=vm(BF16, EMB, n_wide),
        grad_tile=vm(BF16, n_wide, 256),
        scores=vm(F32, n_small // 2, 256, n_wide),
        row_max=vm(F32, 1, longest),
        row_inv=vm(F32, 1, longest),
        ml=vm(F32, nz, ny, 8, ROWS),
        lx=vm(F32, nk, nx, 8, ROWS),
        own_diag=vm(BF16, ROWS, ROWS),
        pos=vm(F32, 1, ROWS),
        send_sem=pltpu.SemaphoreType.DMA((N_REMOTE,)),
        recv_sem=pltpu.SemaphoreType.DMA((N_REMOTE,)),
        load_sem=pltpu.SemaphoreType.DMA((8,)),
    )


class Space:
    def __init__(self, entries):
        self.__dict__.update(entries)


def step_kernel(grid, tree, *refs):
    nz, ny, nx, nk = grid
    n_plane, n_small = nz * ny, nk * nx
    n_tile = n_plane // 2
    n_chunk = n_small // 2
    n_query = n_small * ROWS
    n_wide = n_plane * ROWS
    batch = float(nz * ny * nx * nk * ROWS)
    x_in, lq_in, id_in = refs[0:2], refs[2], refs[3]
    w_in = (refs[4:7], refs[7:10])
    out_ref, loss_ref = refs[10:12]
    s = Space(jax.tree.unflatten(tree, refs[12:]))

    me = lax.axis_index('dp')
    size = grid
    stride = (ny * nx * nk, nx * nk, nk, 1)
    co = tuple(lax.rem(me // stride[ax], size[ax]) for ax in range(4))
    z, y, x, k = co

    def wrap(ax, r):
        return lax.rem(co[ax] + r, size[ax])

    def at_peer(ax, r):
        return me + (wrap(ax, r) - co[ax]) * stride[ax]

    def order(n):
        return sorted(range(1, n), key=lambda r: min(r, n - r))

    used = [0]
    started = []

    class Exchange:
        def __init__(self, peers):
            self.peers = peers
            self.base = used[0]
            used[0] += len(peers)
            self.copies = []

        def send(self, src, dst):
            for i, (r, dest, dev) in enumerate(self.peers):
                copy = pltpu.make_async_remote_copy(
                    src_ref=src(r, dest), dst_ref=dst(r, dest),
                    send_sem=s.send_sem.at[self.base + i], recv_sem=s.recv_sem.at[self.base + i],
                    device_id=(dev,), device_id_type=MESH)
                copy.start()
                self.copies.append(copy)
                started.append(copy)
            return self

        def recv(self):
            for copy in self.copies:
                copy.wait_recv()

    def along(ax):
        return Exchange([(r, wrap(ax, r), at_peer(ax, r)) for r in order(size[ax])])

    def share(ax, ref):
        return along(ax).send(lambda r, d: ref, lambda r, d: ref)

    def small_group():
        peers = []
        for rk in range(nk):
            for rx in [0] + order(nx):
                if rk or rx:
                    dev = me + (wrap(AK, rk) - k) + (wrap(AX, rx) - x) * nk
                    peers.append((len(peers), None, dev))
        return Exchange(peers)

    loads = []

    def load(src, dst):
        copy = pltpu.make_async_copy(src, dst, s.load_sem.at[len(loads)])
        copy.start()
        loads.append(copy)
        return copy

    load_x, load_w = {}, {}
    for t in (1, 0):
        load_x[t] = load(x_in[t], s.xf[t])
        load_w[t] = [load(w_in[t][i], s.wf[t][i]) for i in range(3)]

    barrier = pltpu.get_barrier_semaphore()
    greet = [at_peer(ax, r) for ax in (AZ, AY, AX, AK) for r in range(1, size[ax])]
    greet += [me + (wrap(AK, rk) - k) + (wrap(AX, rx) - x) * nk for rk in range(1, nk) for rx in range(1, nx)]
    for dev in greet:
        pl.semaphore_signal(barrier, inc=1, device_id=(dev,), device_id_type=MESH)

    ids = id_in[...]
    zero_row = jnp.zeros((1, ROWS), F32)
    meta = jnp.concatenate([lq_in[...], lax.shift_right_logical(ids, 16).astype(F32),
                            lax.bitwise_and(ids, 65535).astype(F32)] + [zero_row] * 5, axis=0)
    s.meta_plane[z, y] = meta
    s.meta_small[k, x] = meta

    def forward(t):
        load_x[t].wait()
        xb = s.xf[t][...].astype(BF16)
        for i in range(3):
            load_w[t][i].wait()
            s.wh[t][i][...] = s.wf[t][i][...].astype(BF16)
        act = jnp.maximum(mm(xb, s.wh[t][0][...]), 0.0).astype(BF16)
        s.h1[t][...] = act
        act = jnp.maximum(mm(act, s.wh[t][1][...]), 0.0).astype(BF16)
        s.h2[t][...] = act
        raw = mm(act, s.wh[t][2][...])
        inv = lax.rsqrt(jnp.sum(raw * raw, axis=1, keepdims=True) + NORM_EPS)
        unit = raw * inv
        s.unit[t][...] = unit
        s.inv[t][...] = jnp.broadcast_to(inv, (ROWS, EMB))
        half = unit.astype(BF16)
        s.plane[t][z, y] = half
        s.small[t][k, x] = half

    half_rows = ROWS // 2
    top, low = pl.ds(0, half_rows), pl.ds(half_rows, half_rows)

    def plane_first(t):
        ref = s.plane[t]
        return share(AY, ref.at[z, y, top]), share(AZ, ref.at[z, y, low])

    def plane_second(t, first):
        ref = s.plane[t]
        first[0].recv()
        a = share(AZ, ref.at[z, :, top])
        first[1].recv()
        b = share(AY, ref.at[:, y, low])
        return a, b

    forward(1)
    pl.semaphore_wait(barrier, len(greet))
    v_first = plane_first(1)
    v_small = share(AX, s.small[1].at[k, x])
    meta_y = share(AY, s.meta_plane.at[z, y])
    meta_x = share(AX, s.meta_small.at[k, x])
    forward(0)
    u_small = share(AX, s.small[0].at[k, x])
    v_second = plane_second(1, v_first)
    u_first = plane_first(0)
    meta_y.recv()
    meta_z = share(AZ, s.meta_plane.at[z])
    meta_x.recv()
    meta_k = share(AK, s.meta_small.at[k])
    u_small.recv()
    u_small_k = share(AK, s.small[0].at[k])
    v_small.recv()
    v_small_k = share(AK, s.small[1].at[k])
    u_second = plane_second(0, u_first)

    def columns(ref, lq_out, id_out, id_row, count):
        flat = ref[...].reshape(count * 8, ROWS)
        if count * 8 < ROWS:
            flat = jnp.concatenate([flat, jnp.zeros((ROWS - count * 8, ROWS), F32)], axis=0)
        turned = flat.T
        for i in range(count):
            lq_out[i] = jnp.broadcast_to(turned[:, 8 * i:8 * i + 1], (ROWS, ROWS))
            hi = turned[:, 8 * i + 1:8 * i + 2].astype(jnp.int32)
            lo = turned[:, 8 * i + 2:8 * i + 3].astype(jnp.int32)
            id_out[i] = jnp.broadcast_to(hi * 65536 + lo, (ROWS, ROWS))
            row_hi = flat[8 * i + 1:8 * i + 2].astype(jnp.int32)
            row_lo = flat[8 * i + 2:8 * i + 3].astype(jnp.int32)
            id_row[:, i * ROWS:(i + 1) * ROWS] = row_hi * 65536 + row_lo

    meta_k.recv()
    columns(s.meta_small, s.lqc_small, s.idc_small, s.idr_small, n_small)
    meta_z.recv()
    columns(s.meta_plane, s.lqc_plane, s.idc_plane, s.idr_plane, n_plane)

    def transposed(value):
        return value.astype(F32).T.astype(BF16)

    for t in (0, 1):
        s.xt[t][...] = s.xf[t][...].T.astype(BF16)
        s.h1t[t][...] = transposed(s.h1[t][...])
        s.h2t[t][...] = transposed(s.h2[t][...])

    v_own = s.small[1][k, x]
    u_own = s.small[0][k, x]
    eye = (lax.broadcasted_iota(jnp.int32, (ROWS, ROWS), 0) == lax.broadcasted_iota(jnp.int32, (ROWS, ROWS), 1))
    own_scores = mm(v_own, u_own, C11) * INV_TEMP - s.lqc_small[k * nx + x]
    s.pos[...] = jnp.sum(jnp.where(eye, own_scores, 0.0), axis=0, keepdims=True)

    u_small_k.recv()
    for part in v_second:
        part.recv()

    per_z = ny // 2

    def twice(value):
        return jnp.concatenate([value, value], axis=1)

    def score_tile(tile, carry):
        items = s.plane[1][tile // per_z, pl.ds(lax.rem(tile, per_z) * 2, 2)].reshape(256, EMB)
        lq_wide = twice(s.lqc_plane[pl.ds(tile * 2, 2)].reshape(256, ROWS))
        id_wide = twice(s.idc_plane[pl.ds(tile * 2, 2)].reshape(256, ROWS))
        for n in range(n_chunk):
            lanes = slice(n * 256, (n + 1) * 256)
            queries = s.small[0][2 * n // nx, pl.ds(2 * n % nx, 2)].reshape(256, EMB)
            score = mm(items, queries, C11) * INV_TEMP - lq_wide
            score = jnp.where(id_wide == s.idr_small[:, lanes], -jnp.inf, score)
            peak = jnp.maximum(jnp.max(score, axis=0, keepdims=True), NEG)
            prob = jnp.exp(score - peak)
            s.probs[tile, :, lanes] = prob
            s.tile_max[tile, :, lanes] = peak
            s.tile_sum[tile, :, lanes] = jnp.sum(prob, axis=0, keepdims=True)
        return carry

    lax.fori_loop(0, n_tile, score_tile, 0)

    tile_max = s.tile_max[...]
    part_max = jnp.max(tile_max, axis=0)
    part_sum = jnp.sum(s.tile_sum[...] * jnp.exp(tile_max - part_max[None]), axis=0)
    for i in range(n_small):
        s.stats[k, x, i:i + 1] = part_max[:, i * ROWS:(i + 1) * ROWS]
        s.stats[k, x, n_small + i:n_small + i + 1] = part_sum[:, i * ROWS:(i + 1) * ROWS]
    own_block = k * nx + x
    pos = s.pos[...]
    old_max = s.stats[k, x, pl.ds(own_block, 1)]
    new_max = jnp.maximum(old_max, pos)
    s.stats[k, x, pl.ds(own_block, 1)] = new_max
    s.stats[k, x, pl.ds(n_small + own_block, 1)] = (
        s.stats[k, x, pl.ds(n_small + own_block, 1)] * jnp.exp(old_max - new_max) + jnp.exp(pos - new_max))
    stats_ref = s.stats.at[k, x]
    stats = small_group().send(lambda r, d: stats_ref, lambda r, d: stats_ref)

    for iz in range(nz):
        for iy in range(ny):
            i = iz * ny + iy
            s.plane_t[:, i * ROWS:(i + 1) * ROWS] = transposed(s.plane[1][iz, iy])

    v_small_k.recv()
    for part in u_second:
        part.recv()

    def wide_tile(chunk, carry):
        first = 2 * chunk
        items = s.small[1][first // nx, pl.ds(lax.rem(first, nx), 2)].reshape(256, EMB)
        lq_wide = twice(s.lqc_small[pl.ds(first, 2)].reshape(256, ROWS))
        id_wide = twice(s.idc_small[pl.ds(first, 2)].reshape(256, ROWS))
        for n in range(n_tile):
            lanes = slice(n * 256, (n + 1) * 256)
            queries = s.plane[0][2 * n // ny, pl.ds(2 * n % ny, 2)].reshape(256, EMB)
            score = mm(items, queries, C11) * INV_TEMP - lq_wide
            s.scores[chunk, :, lanes] = jnp.where(id_wide == s.idr_plane[:, lanes], -jnp.inf, score)
        return carry

    lax.fori_loop(0, n_chunk, wide_tile, 0)

    stats.recv()
    every = s.stats[...].reshape(n_small, 2 * n_small, ROWS)
    all_max = jnp.max(every[:, :n_small], axis=0)
    all_sum = jnp.zeros_like(all_max)
    for i in range(n_small):
        all_sum = all_sum + every[i, n_small:] * jnp.exp(every[i, :n_small] - all_max)
    all_inv = 1.0 / (all_sum * batch)
    s.stat_all[:n_small] = all_max
    s.stat_all[n_small:] = all_sum
    for i in range(n_small):
        s.row_max[:, i * ROWS:(i + 1) * ROWS] = all_max[i:i + 1]
        s.row_inv[:, i * ROWS:(i + 1) * ROWS] = all_inv[i:i + 1]
    own_max = s.stat_all[pl.ds(own_block, 1)]
    own_sum = s.stat_all[pl.ds(n_small + own_block, 1)]
    s.ml[z, y] = jnp.concatenate([own_max, own_sum, pos] + [zero_row] * 5, axis=0)
    ml_y = share(AY, s.ml.at[z, y])
    own_grad = (jnp.exp(pos - own_max) / own_sum - 1.0) / batch
    s.own_diag[...] = jnp.where(eye, jnp.broadcast_to(own_grad, (ROWS, ROWS)), 0.0).astype(BF16)

    s.factor[...] = (jnp.exp(tile_max - s.row_max[:, :n_query][None]) * s.row_inv[:, :n_query][None])

    def user_chunk(index, carry):
        chunk = lax.rem((1 - k) * (n_chunk // 2) + index, n_chunk)
        lanes = pl.ds(pl.multiple_of(chunk * 256, 256), 256)
        for tile in range(n_tile):
            s.grad_tile[tile * 256:(tile + 1) * 256] = (
                s.probs[tile, :, lanes] * s.factor[tile, :, lanes]).astype(BF16)
        turned = mm(s.plane_t[...], s.grad_tile[...])
        s.parts[0][2 * chunk] = turned[:, :ROWS]
        s.parts[0][2 * chunk + 1] = turned[:, ROWS:]
        return carry

    def to_partner(t):
        ref = s.parts[t]
        into = s.from_core[t]
        return along(AK).send(lambda r, d: ref.at[pl.ds((1 - k) * nx, nx)], lambda r, d: into)

    def to_x(t, exchange):
        exchange.recv()
        for i in range(nx):
            s.core_sum[t][i] = s.parts[t][k * nx + i] + s.from_core[t][i]
        return along(AX).send(lambda r, d: s.core_sum[t].at[d], lambda r, d: s.from_x[t].at[r - 1])

    def summed(t, exchange):
        exchange.recv()
        total = s.core_sum[t][x]
        for r in range(1, nx):
            total = total + s.from_x[t][r - 1]
        return total * INV_TEMP

    lax.fori_loop(0, n_chunk // 2, user_chunk, 0)
    du_core = to_partner(0)
    lax.fori_loop(n_chunk // 2, n_chunk, user_chunk, 0)
    ml_y.recv()
    ml_z = share(AZ, s.ml.at[z])
    s.parts[0][own_block] = s.parts[0][own_block] + mm(v_own, s.own_diag[...], C00)
    du_x = to_x(0, du_core)

    ml_z.recv()
    loss_row = jnp.zeros((1, ROWS), F32)
    for iz in range(nz):
        for iy in range(ny):
            i = iz * ny + iy
            row = s.ml[iz, iy]
            s.row_max[:, i * ROWS:(i + 1) * ROWS] = row[0:1]
            s.row_inv[:, i * ROWS:(i + 1) * ROWS] = 1.0 / (row[1:2] * batch)
            loss_row = loss_row + ((row[0:1] - row[2:3]) + jnp.log(row[1:2]))
    s.lx[k, x] = jnp.broadcast_to(loss_row, (8, ROWS))
    lx_ref = s.lx.at[k, x]
    loss_x = small_group().send(lambda r, d: lx_ref, lambda r, d: lx_ref)

    def item_chunk(index, carry):
        chunk = lax.rem((1 - k) * (n_chunk // 2) + index, n_chunk)
        total = jnp.zeros((256, EMB), F32)
        grads = []
        for n in range(n_tile):
            lanes = slice(n * 256, (n + 1) * 256)
            grads.append((jnp.exp(s.scores[chunk, :, lanes] - s.row_max[:, lanes])
                          * s.row_inv[:, lanes]).astype(BF16))
        total = mm(jnp.concatenate(grads, axis=1), s.plane[0][...].reshape(n_wide, EMB))
        s.parts[1][2 * chunk] = total[:ROWS]
        s.parts[1][2 * chunk + 1] = total[ROWS:]
        return carry

    lax.fori_loop(0, n_chunk // 2, item_chunk, 0)
    dv_core = to_partner(1)
    lax.fori_loop(n_chunk // 2, n_chunk, item_chunk, 0)
    s.parts[1][own_block] = s.parts[1][own_block] + mm(s.own_diag[...], u_own)
    dv_x = to_x(1, dv_core)

    def backward(t, grad_unit):
        unit = s.unit[t][...]
        grad_raw = s.inv[t][...] * (grad_unit - unit * jnp.sum(unit * grad_unit, axis=1, keepdims=True))
        grad_half = grad_raw.astype(BF16)
        dw = s.dw[t]
        back = mm(grad_half, s.wh[t][2][...], C11)
        grad_two = jnp.where(s.h2[t][...] > 0, back, 0.0).astype(BF16)
        back = mm(grad_two, s.wh[t][1][...], C11)
        grad_one = jnp.where(s.h1[t][...] > 0, back, 0.0).astype(BF16)
        third = mm(s.h2t[t][...], grad_half)
        for i in range(3):
            dw[0, 2, :, i * EMB:(i + 1) * EMB] = third[i * ROWS:(i + 1) * ROWS]
        second = mm(s.h1t[t][...], grad_two)
        for i in range(3):
            dw[1, i] = second[i * ROWS:(i + 1) * ROWS]
        first = mm(s.xt[t][...], grad_one)
        for i in range(2):
            dw[0, i] = first[i * ROWS:(i + 1) * ROWS]

    axes = ((AX, AY, AZ), (AY, AZ, AX), (AZ, AX, AY))

    class WeightSum:
        def __init__(self, t):
            self.t = t

        def rows(self, q, deep):
            a, b, _ = axes[q]
            high = ROWS // size[a]
            if not deep:
                return pl.ds(pl.multiple_of(co[a] * high, high), high)
            step = high // size[b]
            return pl.ds(pl.multiple_of(co[a] * high + co[b] * step, step), step)

        def pair(self):
            ref, into = s.dw[self.t], s.from_pair[self.t]
            self.open = [along(AK).send(lambda r, d: ref.at[1 - k], lambda r, d: into)]

        def close(self):
            for exchange in self.open:
                exchange.recv()

        def scatter_one(self):
            self.close()
            self.open = []
            for q in range(3):
                total = s.pair_sum[self.t]
                total[q] = s.dw[self.t][k, q] + s.from_pair[self.t][q]
                high = ROWS // size[axes[q][0]]
                self.open.append(along(axes[q][0]).send(
                    lambda r, d, q=q, high=high: total.at[q, pl.ds(pl.multiple_of(d * high, high), high)],
                    lambda r, d, q=q: s.ra[self.t][q].at[r - 1]))

        def scatter_two(self):
            done, self.open = self.open, []
            for q in range(3):
                done[q].recv()
                value = s.pair_sum[self.t][q, self.rows(q, False)]
                for r in range(size[axes[q][0]] - 1):
                    value = value + s.ra[self.t][q][r]
                s.sa[self.t][q][...] = value
                step = ROWS // size[axes[q][0]] // size[axes[q][1]]
                self.open.append(along(axes[q][1]).send(
                    lambda r, d, q=q, step=step: s.sa[self.t][q].at[pl.ds(pl.multiple_of(d * step, step), step)],
                    lambda r, d, q=q: s.rb[self.t][q].at[r - 1]))

        def exchange_three(self):
            done, self.open = self.open, []
            for q in range(3):
                done[q].recv()
                a, b, c = axes[q]
                step = ROWS // size[a] // size[b]
                value = s.sa[self.t][q][pl.ds(pl.multiple_of(co[b] * step, step), step)]
                for r in range(size[b] - 1):
                    value = value + s.rb[self.t][q][r]
                s.cx[self.t][q][co[c]] = value
                self.open.append(share(c, s.cx[self.t][q].at[co[c]]))

        def gather_two(self):
            done, self.open = self.open, []
            for q in range(3):
                done[q].recv()
                value = s.cx[self.t][q][0]
                for r in range(1, size[axes[q][2]]):
                    value = value + s.cx[self.t][q][r]
                s.res[k, self.t, q, self.rows(q, True)] = value
                self.open.append(share(axes[q][1], s.res.at[k, self.t, q, self.rows(q, True)]))

        def gather_one(self):
            done, self.open = self.open, []
            for q in range(3):
                done[q].recv()
                self.open.append(share(axes[q][0], s.res.at[k, self.t, q, self.rows(q, False)]))

        def hand_over(self):
            done, self.open = self.open, []
            for q in range(3):
                done[q].recv()
                self.open.append(share(AK, s.res.at[k, self.t, q]))

    user, item = WeightSum(0), WeightSum(1)
    backward(0, summed(0, du_x).T)
    user.pair()
    user.scatter_one()
    backward(1, summed(1, dv_x))
    item.pair()
    user.scatter_two()
    item.scatter_one()
    user.exchange_three()
    item.scatter_two()
    user.gather_two()
    item.exchange_three()
    user.gather_one()
    item.gather_two()
    user.hand_over()
    item.gather_one()
    loss_x.recv()
    loss_total = jnp.zeros((8, ROWS), F32)
    for ik in range(nk):
        for ix in range(nx):
            loss_total = loss_total + s.lx[ik, ix]
    loss_ref[...] = loss_total
    user.close()
    out_ref[:, 0] = s.res[:, 0]
    item.hand_over()
    item.close()
    out_ref[:, 1] = s.res[:, 1]
    for copy in started:
        copy.wait_send()


def finish_kernel(batch, res_ref, loss_in, loss_ref, *outs):
    loss_ref[...] = jnp.sum(loss_in[0:1], axis=1, keepdims=True) / batch
    for t in range(2):
        one, two, three = outs[3 * t:3 * t + 3]
        for i in range(2):
            one[i * ROWS:(i + 1) * ROWS] = res_ref[0, t, i]
        for i in range(3):
            two[i * ROWS:(i + 1) * ROWS] = res_ref[1, t, i]
            three[i * ROWS:(i + 1) * ROWS] = res_ref[0, t, 2, :, i * EMB:(i + 1) * EMB]


def solution(mesh):
    devices = mesh.shape['dp']
    grid = GRIDS[devices]
    scratch, tree = jax.tree.flatten(scratch_table(*grid))
    vmem = pl.BlockSpec(memory_space=pltpu.VMEM)
    anywhere = pl.BlockSpec(memory_space=pl.ANY)

    def device_step(user_x, item_x, item_id, log_q, user_w1, user_w2, user_w3, item_w1, item_w2, item_w3):
        res, loss_rows = pl.pallas_call(
            functools.partial(step_kernel, grid, tree),
            out_shape=(jax.ShapeDtypeStruct((grid[3], 2, 3, ROWS, WIDE), F32), jax.ShapeDtypeStruct((8, ROWS), F32)),
            in_specs=[anywhere, anywhere, vmem, vmem] + [anywhere] * 6,
            out_specs=(vmem, vmem),
            scratch_shapes=scratch,
            compiler_params=pltpu.CompilerParams(collective_id=0, has_side_effects=True, vmem_limit_bytes=60 * 1024 * 1024),
            name='train_step',
        )(user_x, item_x, log_q.reshape(1, ROWS), item_id.reshape(1, ROWS), user_w1, user_w2, user_w3, item_w1, item_w2, item_w3)
        shapes = [(IN_WIDTH, WIDE), (WIDE, WIDE), (WIDE, EMB)] * 2
        outs = pl.pallas_call(
            functools.partial(finish_kernel, float(devices * ROWS)),
            out_shape=[jax.ShapeDtypeStruct((1, 1), F32)] + [jax.ShapeDtypeStruct(shape, F32) for shape in shapes],
            in_specs=[vmem, vmem],
            out_specs=[vmem] * 7,
            name='finish',
        )(res, loss_rows)
        return (outs[0].reshape(()),) + tuple(outs[1:])

    rows, vec, whole = P('dp', None), P('dp'), P()
    return jax.shard_map(device_step, mesh=mesh, in_specs=(rows, rows, vec, vec) + (whole,) * 6,
                         out_specs=(whole,) * 7, check_vma=False)
```

```python
import functools

import jax
import jax.numpy as jnp
from jax import lax
from jax.experimental import pallas as pl
from jax.experimental.pallas import tpu as pltpu
from jax.sharding import PartitionSpec as P

MESH = pl.DeviceIdType.MESH
F32 = jnp.float32
BF16 = jnp.bfloat16
INV_TEMP = 1.0 / 0.05
NORM_EPS = 1e-6
ROWS = 128
EMB = 128
WIDE = 384
IN_WIDTH = 256
NEG = -3.0e38
GRIDS = {128: (4, 4, 4, 2), 16: (2, 2, 2, 2)}
AZ, AY, AX, AK = range(4)
C00 = (((0,), (0,)), ((), ()))
C11 = (((1,), (1,)), ((), ()))
C10 = (((1,), (0,)), ((), ()))
N_REMOTE = 192


def mm(a, b, dims=C10):
    return lax.dot_general(a, b, dims, preferred_element_type=F32)


def scratch_table(nz, ny, nx, nk):
    n_plane, n_small = nz * ny, nk * nx
    n_tile, tile_rows = nz + ny, ny * ROWS // 2
    n_query = n_small * ROWS
    n_wide = n_plane * ROWS
    longest = max(n_wide, n_query)
    turns = ((nx, ny, nz), (ny, nz, nx), (nz, nx, ny))

    def vm(dtype, *shape):
        return pltpu.VMEM(shape, dtype)

    def two(dtype, *shape):
        return [vm(dtype, *shape) for _ in range(2)]

    def six(shape_of):
        return [[vm(F32, *shape_of(*turn), WIDE) for turn in turns] for _ in range(2)]

    return dict(
        xf=two(F32, ROWS, IN_WIDTH),
        wf=[[vm(F32, IN_WIDTH, WIDE), vm(F32, WIDE, WIDE), vm(F32, WIDE, EMB)] for _ in range(2)],
        wh=[[vm(BF16, IN_WIDTH, WIDE), vm(BF16, WIDE, WIDE), vm(BF16, WIDE, EMB)] for _ in range(2)],
        xt=two(BF16, IN_WIDTH, ROWS),
        h1=two(BF16, ROWS, WIDE),
        h2=two(BF16, ROWS, WIDE),
        h1t=two(BF16, WIDE, ROWS),
        h2t=two(BF16, WIDE, ROWS),
        unit=two(F32, ROWS, EMB),
        inv=two(F32, ROWS, EMB),
        plane=two(BF16, nz, ny, ROWS, EMB),
        small=two(BF16, nk, nx, ROWS, EMB),
        parts=two(F32, n_small, ROWS, EMB),
        from_core=two(F32, nx, ROWS, EMB),
        core_sum=two(F32, nx, ROWS, EMB),
        from_x=two(F32, nx - 1, ROWS, EMB),
        dw=two(F32, nk, 3, ROWS, WIDE),
        from_pair=two(F32, 3, ROWS, WIDE),
        pair_sum=two(F32, 3, ROWS, WIDE),
        ra=six(lambda a, b, c: (a - 1, ROWS // a)),
        sa=six(lambda a, b, c: (ROWS // a,)),
        rb=six(lambda a, b, c: (b - 1, ROWS // a // b)),
        cx=six(lambda a, b, c: (c, ROWS // a // b)),
        meta_plane=vm(F32, nz, ny, 8, ROWS),
        meta_small=vm(F32, nk, nx, 8, ROWS),
        lqc_plane=vm(F32, nz, ny, ROWS, ROWS),
        idc_plane=vm(jnp.int32, nz, ny, ROWS, ROWS),
        lqc_small=vm(F32, n_small, ROWS, ROWS),
        idc_small=vm(jnp.int32, n_small, ROWS, ROWS),
        idr_plane=vm(jnp.int32, 1, n_wide),
        idr_small=vm(jnp.int32, 1, n_query),
        probs=vm(F32, n_tile, tile_rows, n_query),
        tile_max=vm(F32, n_tile, 1, n_query),
        tile_sum=vm(F32, n_tile, 1, n_query),
        factor=vm(F32, n_tile, 1, n_query),
        stats=vm(F32, nk, nx, 2 * n_small, ROWS),
        stat_all=vm(F32, 2 * n_small, ROWS),
        plane_t=vm(BF16, EMB, n_wide),
        grad_tile=vm(BF16, n_wide, 256),
        scores=vm(F32, n_small // 2, 256, n_wide),
        row_max=vm(F32, 1, longest),
        row_inv=vm(F32, 1, longest),
        ml=vm(F32, nz, ny, 8, ROWS),
        lx=vm(F32, nk, nx, 8, ROWS),
        own_diag=vm(BF16, ROWS, ROWS),
        pos=vm(F32, 1, ROWS),
        send_sem=pltpu.SemaphoreType.DMA((N_REMOTE,)),
        recv_sem=pltpu.SemaphoreType.DMA((N_REMOTE,)),
        load_sem=pltpu.SemaphoreType.DMA((8,)),
    )


class Space:
    def __init__(self, entries):
        self.__dict__.update(entries)


def step_kernel(grid, tree, *refs):
    nz, ny, nx, nk = grid
    n_plane, n_small = nz * ny, nk * nx
    n_tile, tile_rows = nz + ny, ny * ROWS // 2
    n_chunk = n_small // 2
    n_query = n_small * ROWS
    n_wide = n_plane * ROWS
    batch = float(nz * ny * nx * nk * ROWS)
    x_in, lq_in, id_in = refs[0:2], refs[2], refs[3]
    w_in = (refs[4:7], refs[7:10])
    out_ref, loss_ref = refs[10:12]
    s = Space(jax.tree.unflatten(tree, refs[12:]))

    me = lax.axis_index('dp')
    size = grid
    stride = (ny * nx * nk, nx * nk, nk, 1)
    co = tuple(lax.rem(me // stride[ax], size[ax]) for ax in range(4))
    z, y, x, k = co

    def wrap(ax, r):
        return lax.rem(co[ax] + r, size[ax])

    def at_peer(ax, r):
        return me + (wrap(ax, r) - co[ax]) * stride[ax]

    def order(n):
        return sorted(range(1, n), key=lambda r: min(r, n - r))

    used = [0]
    started = []
    drained = [0]

    class Exchange:
        def __init__(self, peers):
            self.peers = peers
            self.base = used[0]
            used[0] += len(peers)
            self.copies = {}

        def post(self, index, src, dst):
            copy = pltpu.make_async_remote_copy(
                src_ref=src, dst_ref=dst,
                send_sem=s.send_sem.at[self.base + index], recv_sem=s.recv_sem.at[self.base + index],
                device_id=(self.peers[index][2],), device_id_type=MESH)
            copy.start()
            self.copies[index] = copy
            started.append(copy)

        def send(self, src, dst):
            for i, (r, dest, dev) in enumerate(self.peers):
                self.post(i, src(r, dest), dst(r, dest))
            return self

        def recv(self):
            for copy in self.copies.values():
                copy.wait_recv()

        def one(self, index, view):
            return pltpu.make_async_remote_copy(
                src_ref=view, dst_ref=view,
                send_sem=s.send_sem.at[self.base + index], recv_sem=s.recv_sem.at[self.base + index],
                device_id=(self.peers[0][2],), device_id_type=MESH)

    def along(ax):
        return Exchange([(r, wrap(ax, r), at_peer(ax, r)) for r in order(size[ax])])

    def share(ax, ref):
        return along(ax).send(lambda r, d: ref, lambda r, d: ref)

    def small_group():
        peers = []
        for rk in range(nk):
            for rx in [0] + order(nx):
                if rk or rx:
                    dev = me + (wrap(AK, rk) - k) + (wrap(AX, rx) - x) * nk
                    peers.append((len(peers), None, dev))
        return Exchange(peers)

    def plane_group():
        peers = []
        for rz in [0] + order(nz):
            for ry in [0] + order(ny):
                if rz or ry:
                    peers.append((len(peers), None, me + (wrap(AZ, rz) - z) * stride[AZ] + (wrap(AY, ry) - y) * stride[AY]))
        return Exchange(peers)

    def drain(upto):
        while drained[0] < upto:
            started[drained[0]].wait_send()
            drained[0] += 1

    loads = []

    def load(src, dst):
        copy = pltpu.make_async_copy(src, dst, s.load_sem.at[len(loads)])
        copy.start()
        loads.append(copy)
        return copy

    load_x, load_w = {}, {}
    for t in (1, 0):
        load_x[t] = load(x_in[t], s.xf[t])
        load_w[t] = [load(w_in[t][i], s.wf[t][i]) for i in range(3)]

    barrier = pltpu.get_barrier_semaphore()
    greet = [at_peer(ax, r) for ax in (AZ, AY, AX, AK) for r in range(1, size[ax])]
    greet += [me + (wrap(AK, rk) - k) + (wrap(AX, rx) - x) * nk for rk in range(1, nk) for rx in range(1, nx)]
    greet += [me + (wrap(AZ, rz) - z) * stride[AZ] + (wrap(AY, ry) - y) * stride[AY] for rz in range(1, nz) for ry in range(1, ny)]
    for dev in greet:
        pl.semaphore_signal(barrier, inc=1, device_id=(dev,), device_id_type=MESH)

    ids = id_in[...]
    zero_row = jnp.zeros((1, ROWS), F32)
    meta = jnp.concatenate([lq_in[...], lax.shift_right_logical(ids, 16).astype(F32),
                            lax.bitwise_and(ids, 65535).astype(F32)] + [zero_row] * 5, axis=0)
    s.meta_plane[z, y] = meta
    s.meta_small[k, x] = meta

    def forward(t):
        load_x[t].wait()
        xb = s.xf[t][...].astype(BF16)
        for i in range(3):
            load_w[t][i].wait()
            s.wh[t][i][...] = s.wf[t][i][...].astype(BF16)
        act = jnp.maximum(mm(xb, s.wh[t][0][...]), 0.0).astype(BF16)
        s.h1[t][...] = act
        act = jnp.maximum(mm(act, s.wh[t][1][...]), 0.0).astype(BF16)
        s.h2[t][...] = act
        raw = mm(act, s.wh[t][2][...])
        inv = lax.rsqrt(jnp.sum(raw * raw, axis=1, keepdims=True) + NORM_EPS)
        unit = raw * inv
        s.unit[t][...] = unit
        s.inv[t][...] = jnp.broadcast_to(inv, (ROWS, EMB))
        half = unit.astype(BF16)
        s.plane[t][z, y] = half
        s.small[t][k, x] = half

    half_rows = ROWS // 2
    top, low = pl.ds(0, half_rows), pl.ds(half_rows, half_rows)

    def plane_first(t):
        ref = s.plane[t]
        return share(AY, ref.at[z, y, top]), share(AZ, ref.at[z, y, low])

    def plane_second(t, first):
        ref = s.plane[t]
        first[0].recv()
        a = share(AZ, ref.at[z, :, top])
        first[1].recv()
        b = share(AY, ref.at[:, y, low])
        return a, b

    forward(1)
    pl.semaphore_wait(barrier, len(greet))
    v_first = plane_first(1)
    v_small = share(AX, s.small[1].at[k, x])
    meta_y = share(AY, s.meta_plane.at[z, y])
    meta_x = share(AX, s.meta_small.at[k, x])
    forward(0)
    u_small = share(AX, s.small[0].at[k, x])
    u_first = plane_first(0)
    v_second = plane_second(1, v_first)
    meta_y.recv()
    meta_z = share(AZ, s.meta_plane.at[z])
    meta_x.recv()
    meta_k = share(AK, s.meta_small.at[k])
    u_small.recv()
    u_small_k = share(AK, s.small[0].at[k])
    u_second = plane_second(0, u_first)
    v_small.recv()
    v_small_k = share(AK, s.small[1].at[k])
    gathers = len(started)

    def columns(ref, lq_out, id_out, id_row, count, nested):
        flat = ref[...].reshape(count * 8, ROWS)
        if count * 8 < ROWS:
            flat = jnp.concatenate([flat, jnp.zeros((ROWS - count * 8, ROWS), F32)], axis=0)
        turned = flat.T
        for i in range(count):
            lq_out[divmod(i, nested) if nested else i] = jnp.broadcast_to(turned[:, 8 * i:8 * i + 1], (ROWS, ROWS))
            hi = turned[:, 8 * i + 1:8 * i + 2].astype(jnp.int32)
            lo = turned[:, 8 * i + 2:8 * i + 3].astype(jnp.int32)
            id_out[divmod(i, nested) if nested else i] = jnp.broadcast_to(hi * 65536 + lo, (ROWS, ROWS))
            row_hi = flat[8 * i + 1:8 * i + 2].astype(jnp.int32)
            row_lo = flat[8 * i + 2:8 * i + 3].astype(jnp.int32)
            id_row[:, i * ROWS:(i + 1) * ROWS] = row_hi * 65536 + row_lo

    meta_k.recv()
    columns(s.meta_small, s.lqc_small, s.idc_small, s.idr_small, n_small, 0)
    meta_z.recv()
    columns(s.meta_plane, s.lqc_plane, s.idc_plane, s.idr_plane, n_plane, ny)

    def transposed(value):
        return value.astype(F32).T.astype(BF16)

    for t in (0, 1):
        s.xt[t][...] = s.xf[t][...].T.astype(BF16)
        s.h1t[t][...] = transposed(s.h1[t][...])
        s.h2t[t][...] = transposed(s.h2[t][...])

    v_own = s.small[1][k, x]
    u_own = s.small[0][k, x]
    eye = (lax.broadcasted_iota(jnp.int32, (ROWS, ROWS), 0) == lax.broadcasted_iota(jnp.int32, (ROWS, ROWS), 1))
    own_scores = mm(v_own, u_own, C11) * INV_TEMP - s.lqc_small[k * nx + x]
    s.pos[...] = jnp.sum(jnp.where(eye, own_scores, 0.0), axis=0, keepdims=True)

    u_small_k.recv()

    def twice(value):
        return jnp.concatenate([value, value], axis=1)

    def score_tile(slot, items, lq_part, id_part):
        s.plane_t[:, pl.ds(pl.multiple_of(slot * tile_rows, tile_rows), tile_rows)] = transposed(items)
        lq_wide = twice(lq_part.reshape(tile_rows, ROWS))
        id_wide = twice(id_part.reshape(tile_rows, ROWS))
        for n in range(n_chunk):
            lanes = slice(n * 256, (n + 1) * 256)
            queries = s.small[0][2 * n // nx, pl.ds(2 * n % nx, 2)].reshape(256, EMB)
            score = mm(items, queries, C11) * INV_TEMP - lq_wide
            score = jnp.where(id_wide == s.idr_small[:, lanes], -jnp.inf, score)
            peak = jnp.maximum(jnp.max(score, axis=0, keepdims=True), NEG)
            prob = jnp.exp(score - peak)
            s.probs[slot, :, lanes] = prob
            s.tile_max[slot, :, lanes] = peak
            s.tile_sum[slot, :, lanes] = jnp.sum(prob, axis=0, keepdims=True)

    def score_step(index, carry):
        turn = jnp.where(index == 2, 3, jnp.where(index == 3, 2, index))
        ref = s.plane[1]

        @pl.when(index > 0)
        def _():
            for part, view in zip(v_second, (ref.at[z, :, top], ref.at[:, y, low])):
                part.one(index - 1, view).wait_recv()

        iz = lax.rem(z - turn + nz, nz)
        iy = lax.rem(y - turn + ny, ny)
        score_tile(2 * index, ref[iz, :, top].reshape(tile_rows, EMB), s.lqc_plane[iz, :, top], s.idc_plane[iz, :, top])
        score_tile(2 * index + 1, ref[:, iy, low].reshape(tile_rows, EMB), s.lqc_plane[:, iy, low], s.idc_plane[:, iy, low])
        return carry

    lax.fori_loop(0, nz, score_step, 0)

    tile_max = s.tile_max[...]
    part_max = jnp.max(tile_max, axis=0)
    part_sum = jnp.sum(s.tile_sum[...] * jnp.exp(tile_max - part_max[None]), axis=0)
    for i in range(n_small):
        s.stats[k, x, i:i + 1] = part_max[:, i * ROWS:(i + 1) * ROWS]
        s.stats[k, x, n_small + i:n_small + i + 1] = part_sum[:, i * ROWS:(i + 1) * ROWS]
    own_block = k * nx + x
    pos = s.pos[...]
    old_max = s.stats[k, x, pl.ds(own_block, 1)]
    new_max = jnp.maximum(old_max, pos)
    s.stats[k, x, pl.ds(own_block, 1)] = new_max
    s.stats[k, x, pl.ds(n_small + own_block, 1)] = (
        s.stats[k, x, pl.ds(n_small + own_block, 1)] * jnp.exp(old_max - new_max) + jnp.exp(pos - new_max))
    stats_ref = s.stats.at[k, x]
    stats = small_group().send(lambda r, d: stats_ref, lambda r, d: stats_ref)

    v_small_k.recv()
    for part in u_second:
        part.recv()

    stages = ((2, 1), (3, 0)) if nx == 4 else ((1, 0),)

    n_wide_tile = n_wide // 256

    def wide_tile(chunk, carry):
        side = jnp.where(lax.rem(chunk, 2) == 0, 1 - k, k)
        spots = []
        for turns in zip(*stages):
            spots.append(lax.rem(x + jnp.where(chunk // 2 == 0, turns[0], turns[-1]), nx))
        items = jnp.concatenate([s.small[1][side, spot] for spot in spots], axis=0)
        lq_wide = twice(jnp.concatenate([s.lqc_small[side * nx + spot] for spot in spots], axis=0))
        id_wide = twice(jnp.concatenate([s.idc_small[side * nx + spot] for spot in spots], axis=0))
        for n in range(n_wide_tile):
            lanes = slice(n * 256, (n + 1) * 256)
            queries = s.plane[0][2 * n // ny, pl.ds(2 * n % ny, 2)].reshape(256, EMB)
            score = mm(items, queries, C11) * INV_TEMP - lq_wide
            s.scores[chunk, :, lanes] = jnp.where(id_wide == s.idr_plane[:, lanes], -jnp.inf, score)
        return carry

    lax.fori_loop(0, n_chunk, wide_tile, 0)

    stats.recv()
    every = s.stats[...].reshape(n_small, 2 * n_small, ROWS)
    all_max = jnp.max(every[:, :n_small], axis=0)
    all_sum = jnp.zeros_like(all_max)
    for i in range(n_small):
        all_sum = all_sum + every[i, n_small:] * jnp.exp(every[i, :n_small] - all_max)
    all_inv = 1.0 / (all_sum * batch)
    s.stat_all[:n_small] = all_max
    s.stat_all[n_small:] = all_sum
    for i in range(n_small):
        s.row_max[:, i * ROWS:(i + 1) * ROWS] = all_max[i:i + 1]
        s.row_inv[:, i * ROWS:(i + 1) * ROWS] = all_inv[i:i + 1]
    own_max = s.stat_all[pl.ds(own_block, 1)]
    own_sum = s.stat_all[pl.ds(n_small + own_block, 1)]
    s.ml[z, y] = jnp.concatenate([own_max, own_sum, pos] + [zero_row] * 5, axis=0)
    ml_ref = s.ml.at[z, y]
    ml_plane = plane_group().send(lambda r, d: ml_ref, lambda r, d: ml_ref)
    own_grad = (jnp.exp(pos - own_max) / own_sum - 1.0) / batch
    s.own_diag[...] = jnp.where(eye, jnp.broadcast_to(own_grad, (ROWS, ROWS)), 0.0).astype(BF16)

    s.factor[...] = (jnp.exp(tile_max - s.row_max[:, :n_query][None]) * s.row_inv[:, :n_query][None])

    def user_chunk(index, carry):
        chunk = lax.rem((1 - k) * (n_chunk // 2) + index, n_chunk)
        lanes = pl.ds(pl.multiple_of(chunk * 256, 256), 256)
        for tile in range(n_tile):
            s.grad_tile[tile * tile_rows:(tile + 1) * tile_rows] = (
                s.probs[tile, :, lanes] * s.factor[tile, :, lanes]).astype(BF16)
        turned = mm(s.plane_t[...], s.grad_tile[...])
        s.parts[0][2 * chunk] = turned[:, :ROWS]
        s.parts[0][2 * chunk + 1] = turned[:, ROWS:]
        return carry

    def to_partner(t):
        ref = s.parts[t]
        into = s.from_core[t]
        return along(AK).send(lambda r, d: ref.at[pl.ds((1 - k) * nx, nx)], lambda r, d: into)

    def to_x(t, exchange):
        exchange.recv()
        for i in range(nx):
            s.core_sum[t][i] = s.parts[t][k * nx + i] + s.from_core[t][i]
        return along(AX).send(lambda r, d: s.core_sum[t].at[d], lambda r, d: s.from_x[t].at[r - 1])

    def summed(t, exchange):
        exchange.recv()
        total = s.core_sum[t][x]
        for r in range(1, nx):
            total = total + s.from_x[t][r - 1]
        return total * INV_TEMP

    lax.fori_loop(0, n_chunk // 2, user_chunk, 0)
    du_core = to_partner(0)
    lax.fori_loop(n_chunk // 2, n_chunk, user_chunk, 0)
    s.parts[0][own_block] = s.parts[0][own_block] + mm(v_own, s.own_diag[...], C00)
    du_x = to_x(0, du_core)
    drain(gathers)
    ml_plane.recv()
    loss_row = jnp.zeros((1, ROWS), F32)
    for iz in range(nz):
        for iy in range(ny):
            i = iz * ny + iy
            row = s.ml[iz, iy]
            s.row_max[:, i * ROWS:(i + 1) * ROWS] = row[0:1]
            s.row_inv[:, i * ROWS:(i + 1) * ROWS] = 1.0 / (row[1:2] * batch)
            loss_row = loss_row + ((row[0:1] - row[2:3]) + jnp.log(row[1:2]))
    s.lx[k, x] = jnp.broadcast_to(loss_row, (8, ROWS))
    lx_ref = s.lx.at[k, x]
    loss_x = small_group().send(lambda r, d: lx_ref, lambda r, d: lx_ref)

    def item_chunk(stage, side, own):
        chunk = 2 * stage + own
        grads = []
        for n in range(n_wide_tile):
            lanes = slice(n * 256, (n + 1) * 256)
            grads.append((jnp.exp(s.scores[chunk, :, lanes] - s.row_max[:, lanes])
                          * s.row_inv[:, lanes]).astype(BF16))
        total = mm(jnp.concatenate(grads, axis=1), s.plane[0][...].reshape(n_wide, EMB))
        for i, r in enumerate(stages[stage]):
            s.parts[1][side * nx + wrap(AX, r)] = total[i * ROWS:(i + 1) * ROWS]

    dv_core = Exchange([(i, None, at_peer(AK, 1)) for i in range(nx)])
    dv_x = along(AX)
    for stage, turns in enumerate(stages):
        item_chunk(stage, 1 - k, 0)
        for i, r in enumerate(turns):
            spot = wrap(AX, r)
            dv_core.post(2 * stage + i, s.parts[1].at[(1 - k) * nx + spot], s.from_core[1].at[spot])
        item_chunk(stage, k, 1)
        if 0 in turns:
            s.parts[1][own_block] = s.parts[1][own_block] + mm(s.own_diag[...], u_own)
        for i, r in enumerate(turns):
            spot = wrap(AX, r)
            dv_core.copies[2 * stage + i].wait_recv()
            s.core_sum[1][spot] = s.parts[1][k * nx + spot] + s.from_core[1][spot]
            if r:
                dv_x.post(order(nx).index(r), s.core_sum[1].at[spot], s.from_x[1].at[r - 1])
    middle = len(started)

    def backward(t, grad_unit):
        unit = s.unit[t][...]
        grad_raw = s.inv[t][...] * (grad_unit - unit * jnp.sum(unit * grad_unit, axis=1, keepdims=True))
        grad_half = grad_raw.astype(BF16)
        dw = s.dw[t]
        back = mm(grad_half, s.wh[t][2][...], C11)
        grad_two = jnp.where(s.h2[t][...] > 0, back, 0.0).astype(BF16)
        back = mm(grad_two, s.wh[t][1][...], C11)
        grad_one = jnp.where(s.h1[t][...] > 0, back, 0.0).astype(BF16)
        third = mm(s.h2t[t][...], grad_half)
        for i in range(3):
            dw[0, 2, :, i * EMB:(i + 1) * EMB] = third[i * ROWS:(i + 1) * ROWS]
        second = mm(s.h1t[t][...], grad_two)
        for i in range(3):
            dw[1, i] = second[i * ROWS:(i + 1) * ROWS]
        first = mm(s.xt[t][...], grad_one)
        for i in range(2):
            dw[0, i] = first[i * ROWS:(i + 1) * ROWS]

    axes = ((AX, AY, AZ), (AY, AZ, AX), (AZ, AX, AY))

    class WeightSum:
        def __init__(self, t):
            self.t = t

        def rows(self, q, deep):
            a, b, _ = axes[q]
            high = ROWS // size[a]
            if not deep:
                return pl.ds(pl.multiple_of(co[a] * high, high), high)
            step = high // size[b]
            return pl.ds(pl.multiple_of(co[a] * high + co[b] * step, step), step)

        def pair(self):
            ref, into = s.dw[self.t], s.from_pair[self.t]
            self.open = [along(AK).send(lambda r, d: ref.at[1 - k], lambda r, d: into)]

        def close(self):
            for exchange in self.open:
                exchange.recv()

        def scatter_one(self):
            self.close()
            self.open = []
            for q in range(3):
                total = s.pair_sum[self.t]
                total[q] = s.dw[self.t][k, q] + s.from_pair[self.t][q]
                high = ROWS // size[axes[q][0]]
                self.open.append(along(axes[q][0]).send(
                    lambda r, d, q=q, high=high: total.at[q, pl.ds(pl.multiple_of(d * high, high), high)],
                    lambda r, d, q=q: s.ra[self.t][q].at[r - 1]))

        def scatter_two(self):
            done, self.open = self.open, []
            for q in range(3):
                done[q].recv()
                value = s.pair_sum[self.t][q, self.rows(q, False)]
                for r in range(size[axes[q][0]] - 1):
                    value = value + s.ra[self.t][q][r]
                s.sa[self.t][q][...] = value
                step = ROWS // size[axes[q][0]] // size[axes[q][1]]
                self.open.append(along(axes[q][1]).send(
                    lambda r, d, q=q, step=step: s.sa[self.t][q].at[pl.ds(pl.multiple_of(d * step, step), step)],
                    lambda r, d, q=q: s.rb[self.t][q].at[r - 1]))

        def exchange_three(self):
            done, self.open = self.open, []
            for q in range(3):
                done[q].recv()
                a, b, c = axes[q]
                step = ROWS // size[a] // size[b]
                value = s.sa[self.t][q][pl.ds(pl.multiple_of(co[b] * step, step), step)]
                for r in range(size[b] - 1):
                    value = value + s.rb[self.t][q][r]
                s.cx[self.t][q][co[c]] = value
                self.open.append(share(c, s.cx[self.t][q].at[co[c]]))

        def gather_two(self):
            done, self.open = self.open, []
            for q in range(3):
                done[q].recv()
                value = s.cx[self.t][q][0]
                for r in range(1, size[axes[q][2]]):
                    value = value + s.cx[self.t][q][r]
                out_ref[k, self.t, q, self.rows(q, True)] = value
                self.open.append(share(axes[q][1], out_ref.at[k, self.t, q, self.rows(q, True)]))

        def gather_one(self):
            done, self.open = self.open, []
            for q in range(3):
                done[q].recv()
                self.open.append(share(axes[q][0], out_ref.at[k, self.t, q, self.rows(q, False)]))

        def hand_over(self):
            done, self.open = self.open, []
            for q in range(3):
                done[q].recv()
                self.open.append(share(AK, out_ref.at[k, self.t, q]))

    user, item = WeightSum(0), WeightSum(1)
    backward(0, summed(0, du_x).T)
    user.pair()
    user.scatter_one()
    backward(1, summed(1, dv_x))
    item.pair()
    drain(middle)
    user.scatter_two()
    item.scatter_one()
    early = len(started)
    user.exchange_three()
    item.scatter_two()
    drain(early)
    early = len(started)
    user.gather_two()
    item.exchange_three()
    drain(early)
    early = len(started)
    user.gather_one()
    item.gather_two()
    drain(early)
    early = len(started)
    user.hand_over()
    item.gather_one()
    drain(early)
    loss_x.recv()
    loss_total = jnp.zeros((8, ROWS), F32)
    for ik in range(nk):
        for ix in range(nx):
            loss_total = loss_total + s.lx[ik, ix]
    loss_ref[...] = loss_total
    user.close()
    item.hand_over()
    item.close()
    drain(len(started))


def finish_kernel(batch, res_ref, loss_in, loss_ref, *outs):
    loss_ref[...] = jnp.sum(loss_in[0:1], axis=1, keepdims=True) / batch
    for t in range(2):
        one, two, three = outs[3 * t:3 * t + 3]
        for i in range(2):
            one[i * ROWS:(i + 1) * ROWS] = res_ref[0, t, i]
        for i in range(3):
            two[i * ROWS:(i + 1) * ROWS] = res_ref[1, t, i]
            three[i * ROWS:(i + 1) * ROWS] = res_ref[0, t, 2, :, i * EMB:(i + 1) * EMB]


def solution(mesh):
    devices = mesh.shape['dp']
    grid = GRIDS[devices]
    scratch, tree = jax.tree.flatten(scratch_table(*grid))
    vmem = pl.BlockSpec(memory_space=pltpu.VMEM)
    hbm = pl.BlockSpec(memory_space=pltpu.HBM)

    def device_step(user_x, item_x, item_id, log_q, user_w1, user_w2, user_w3, item_w1, item_w2, item_w3):
        res, loss_rows = pl.pallas_call(
            functools.partial(step_kernel, grid, tree),
            out_shape=(jax.ShapeDtypeStruct((grid[3], 2, 3, ROWS, WIDE), F32), jax.ShapeDtypeStruct((8, ROWS), F32)),
            in_specs=[hbm, hbm, vmem, vmem] + [hbm] * 6,
            out_specs=(vmem, vmem),
            scratch_shapes=scratch,
            compiler_params=pltpu.CompilerParams(collective_id=0, has_side_effects=True, vmem_limit_bytes=60 * 1024 * 1024),
            name='train_step',
        )(user_x, item_x, log_q.reshape(1, ROWS), item_id.reshape(1, ROWS), user_w1, user_w2, user_w3, item_w1, item_w2, item_w3)
        shapes = [(IN_WIDTH, WIDE), (WIDE, WIDE), (WIDE, EMB)] * 2
        outs = pl.pallas_call(
            functools.partial(finish_kernel, float(devices * ROWS)),
            out_shape=[jax.ShapeDtypeStruct((1, 1), F32)] + [jax.ShapeDtypeStruct(shape, F32) for shape in shapes],
            in_specs=[vmem, vmem],
            out_specs=[vmem] * 7,
            name='finish',
        )(res, loss_rows)
        return (outs[0].reshape(()),) + tuple(outs[1:])

    rows, vec, whole = P('dp', None), P('dp'), P()
    return jax.shard_map(device_step, mesh=mesh, in_specs=(rows, rows, vec, vec) + (whole,) * 6,
                         out_specs=(whole,) * 7, check_vma=False)
```

```python
import functools

import jax
import jax.numpy as jnp
from jax import lax
from jax.experimental import pallas as pl
from jax.experimental.pallas import tpu as pltpu
from jax.sharding import PartitionSpec as P

MESH = pl.DeviceIdType.MESH
F32 = jnp.float32
BF16 = jnp.bfloat16
INV_TEMP = 1.0 / 0.05
NORM_EPS = 1e-6
ROWS = 128
EMB = 128
WIDE = 384
IN_WIDTH = 256
NEG = -3.0e38
GRIDS = {128: (4, 4, 4, 2), 16: (2, 2, 2, 2)}
AZ, AY, AX, AK = range(4)
C00 = (((0,), (0,)), ((), ()))
C11 = (((1,), (1,)), ((), ()))
C10 = (((1,), (0,)), ((), ()))
N_REMOTE = 192


def mm(a, b, dims=C10):
    return lax.dot_general(a, b, dims, preferred_element_type=F32)


def scratch_table(nz, ny, nx, nk):
    n_plane, n_small = nz * ny, nk * nx
    n_tile, tile_rows = nz + ny, ny * ROWS // 2
    n_query = n_small * ROWS
    n_wide = n_plane * ROWS
    longest = max(n_wide, n_query)
    turns = ((nx, ny, nz), (ny, nz, nx), (nz, nx, ny))

    def vm(dtype, *shape):
        return pltpu.VMEM(shape, dtype)

    def two(dtype, *shape):
        return [vm(dtype, *shape) for _ in range(2)]

    def each(shape_of):
        return [vm(F32, *shape_of(*turn), WIDE) for turn in turns]

    return dict(
        wh=[[vm(BF16, IN_WIDTH, WIDE), vm(BF16, WIDE, WIDE), vm(BF16, WIDE, EMB)] for _ in range(2)],
        h1=two(BF16, ROWS, WIDE),
        h2=two(BF16, ROWS, WIDE),
        xt=vm(BF16, 2, nk, IN_WIDTH, ROWS),
        h1t=vm(BF16, 2, nk, WIDE, ROWS),
        h2t=vm(BF16, 2, nk, WIDE, ROWS),
        g1=vm(BF16, 2, nk, ROWS, WIDE),
        g2=vm(BF16, 2, nk, ROWS, WIDE),
        g3=vm(BF16, 2, nk, ROWS, EMB),
        unit=two(F32, ROWS, EMB),
        inv=two(F32, ROWS, EMB),
        plane=two(BF16, nz, ny, ROWS, EMB),
        small=two(BF16, nk, nx, ROWS, EMB),
        parts=two(F32, n_small, ROWS, EMB),
        from_core=two(F32, nx, ROWS, EMB),
        core_sum=two(F32, nx, ROWS, EMB),
        from_x=two(F32, nx - 1, ROWS, EMB),
        dw=vm(F32, 3, 2, ROWS, WIDE),
        ra=each(lambda a, b, c: (a - 1, 2, ROWS // a)),
        sa=each(lambda a, b, c: (2, ROWS // a)),
        rb=each(lambda a, b, c: (b - 1, 2, ROWS // a // b)),
        cx=each(lambda a, b, c: (c, 2, ROWS // a // b)),
        meta_plane=vm(F32, nz, ny, 8, ROWS),
        meta_small=vm(F32, nk, nx, 8, ROWS),
        lqc_plane=vm(F32, nz, ny, ROWS, ROWS),
        idc_plane=vm(jnp.int32, nz, ny, ROWS, ROWS),
        lqc_small=vm(F32, n_small, ROWS, ROWS),
        idc_small=vm(jnp.int32, n_small, ROWS, ROWS),
        idr_plane=vm(jnp.int32, 1, n_wide),
        idr_small=vm(jnp.int32, 1, n_query),
        probs=vm(F32, n_tile, tile_rows, n_query),
        tile_max=vm(F32, n_tile, 1, n_query),
        tile_sum=vm(F32, n_tile, 1, n_query),
        factor=vm(F32, n_tile, 1, n_query),
        stats=vm(F32, nk, nx, 2 * n_small, ROWS),
        stat_all=vm(F32, 2 * n_small, ROWS),
        plane_t=vm(BF16, EMB, n_wide),
        grad_tile=vm(BF16, n_wide, 256),
        scores=vm(F32, n_small // 2, 256, n_wide),
        row_max=vm(F32, 1, longest),
        row_inv=vm(F32, 1, longest),
        ml=vm(F32, nz, ny, 8, ROWS),
        lx=vm(F32, nk, nx, 8, ROWS),
        own_diag=vm(BF16, ROWS, ROWS),
        pos=vm(F32, 1, ROWS),
        send_sem=pltpu.SemaphoreType.DMA((N_REMOTE,)),
        recv_sem=pltpu.SemaphoreType.DMA((N_REMOTE,)),
    )


class Space:
    def __init__(self, entries):
        self.__dict__.update(entries)


def step_kernel(grid, tree, *refs):
    nz, ny, nx, nk = grid
    n_plane, n_small = nz * ny, nk * nx
    n_tile, tile_rows = nz + ny, ny * ROWS // 2
    n_chunk = n_small // 2
    n_query = n_small * ROWS
    n_wide = n_plane * ROWS
    batch = float(nz * ny * nx * nk * ROWS)
    x_in, lq_in, id_in = refs[0:2], refs[2], refs[3]
    w_in = (refs[4:7], refs[7:10])
    out_ref, loss_ref = refs[10:12]
    s = Space(jax.tree.unflatten(tree, refs[12:]))

    me = lax.axis_index('dp')
    size = grid
    stride = (ny * nx * nk, nx * nk, nk, 1)
    co = tuple(lax.rem(me // stride[ax], size[ax]) for ax in range(4))
    z, y, x, k = co

    def wrap(ax, r):
        return lax.rem(co[ax] + r, size[ax])

    def at_peer(ax, r):
        return me + (wrap(ax, r) - co[ax]) * stride[ax]

    def order(n):
        return sorted(range(1, n), key=lambda r: min(r, n - r))

    used = [0]
    started = []
    drained = [0]

    class Exchange:
        def __init__(self, peers):
            self.peers = peers
            self.base = used[0]
            used[0] += len(peers)
            self.copies = {}

        def post(self, index, src, dst):
            copy = pltpu.make_async_remote_copy(
                src_ref=src, dst_ref=dst,
                send_sem=s.send_sem.at[self.base + index], recv_sem=s.recv_sem.at[self.base + index],
                device_id=(self.peers[index][2],), device_id_type=MESH)
            copy.start()
            self.copies[index] = copy
            started.append(copy)

        def send(self, src, dst):
            for i, (r, dest, dev) in enumerate(self.peers):
                self.post(i, src(r, dest), dst(r, dest))
            return self

        def recv(self):
            for copy in self.copies.values():
                copy.wait_recv()

        def one(self, index, view):
            return pltpu.make_async_remote_copy(
                src_ref=view, dst_ref=view,
                send_sem=s.send_sem.at[self.base + index], recv_sem=s.recv_sem.at[self.base + index],
                device_id=(self.peers[0][2],), device_id_type=MESH)

    def along(ax):
        return Exchange([(r, wrap(ax, r), at_peer(ax, r)) for r in order(size[ax])])

    def share(ax, ref):
        return along(ax).send(lambda r, d: ref, lambda r, d: ref)

    def small_group():
        peers = []
        for rk in range(nk):
            for rx in [0] + order(nx):
                if rk or rx:
                    dev = me + (wrap(AK, rk) - k) + (wrap(AX, rx) - x) * nk
                    peers.append((len(peers), None, dev))
        return Exchange(peers)

    def plane_group():
        peers = []
        for rz in [0] + order(nz):
            for ry in [0] + order(ny):
                if rz or ry:
                    peers.append((len(peers), None, me + (wrap(AZ, rz) - z) * stride[AZ] + (wrap(AY, ry) - y) * stride[AY]))
        return Exchange(peers)

    def drain(upto):
        while drained[0] < upto:
            started[drained[0]].wait_send()
            drained[0] += 1

    barrier = pltpu.get_barrier_semaphore()
    greet = [at_peer(ax, r) for ax in (AZ, AY, AX, AK) for r in range(1, size[ax])]
    greet += [me + (wrap(AK, rk) - k) + (wrap(AX, rx) - x) * nk for rk in range(1, nk) for rx in range(1, nx)]
    greet += [me + (wrap(AZ, rz) - z) * stride[AZ] + (wrap(AY, ry) - y) * stride[AY] for rz in range(1, nz) for ry in range(1, ny)]
    for dev in greet:
        pl.semaphore_signal(barrier, inc=1, device_id=(dev,), device_id_type=MESH)

    ids = id_in[...]
    zero_row = jnp.zeros((1, ROWS), F32)
    meta = jnp.concatenate([lq_in[...], lax.shift_right_logical(ids, 16).astype(F32),
                            lax.bitwise_and(ids, 65535).astype(F32)] + [zero_row] * 5, axis=0)
    s.meta_plane[z, y] = meta
    s.meta_small[k, x] = meta

    def forward(t):
        xb = x_in[t][...].astype(BF16)
        for i in range(3):
            s.wh[t][i][...] = w_in[t][i][...].astype(BF16)
        act = jnp.maximum(mm(xb, s.wh[t][0][...]), 0.0).astype(BF16)
        s.h1[t][...] = act
        act = jnp.maximum(mm(act, s.wh[t][1][...]), 0.0).astype(BF16)
        s.h2[t][...] = act
        raw = mm(act, s.wh[t][2][...])
        inv = lax.rsqrt(jnp.sum(raw * raw, axis=1, keepdims=True) + NORM_EPS)
        unit = raw * inv
        s.unit[t][...] = unit
        s.inv[t][...] = jnp.broadcast_to(inv, (ROWS, EMB))
        half = unit.astype(BF16)
        s.plane[t][z, y] = half
        s.small[t][k, x] = half

    half_rows = ROWS // 2
    top, low = pl.ds(0, half_rows), pl.ds(half_rows, half_rows)

    def plane_first(t):
        ref = s.plane[t]
        return share(AY, ref.at[z, y, top]), share(AZ, ref.at[z, y, low])

    def plane_second(t, first):
        ref = s.plane[t]
        first[0].recv()
        a = share(AZ, ref.at[z, :, top])
        first[1].recv()
        b = share(AY, ref.at[:, y, low])
        return a, b

    forward(1)
    pl.semaphore_wait(barrier, len(greet))
    meta_y = share(AY, s.meta_plane.at[z, y])
    meta_x = share(AX, s.meta_small.at[k, x])
    v_first = plane_first(1)
    v_small = share(AX, s.small[1].at[k, x])
    forward(0)
    u_small = share(AX, s.small[0].at[k, x])
    u_first = plane_first(0)
    meta_y.recv()
    meta_z = share(AZ, s.meta_plane.at[z])
    meta_x.recv()
    meta_k = share(AK, s.meta_small.at[k])
    v_second = plane_second(1, v_first)
    u_small.recv()
    u_small_k = share(AK, s.small[0].at[k])
    u_second = plane_second(0, u_first)
    v_small.recv()
    v_small_k = share(AK, s.small[1].at[k])

    def columns(ref, lq_out, id_out, id_row, count, nested):
        flat = ref[...].reshape(count * 8, ROWS)
        if count * 8 < ROWS:
            flat = jnp.concatenate([flat, jnp.zeros((ROWS - count * 8, ROWS), F32)], axis=0)
        turned = flat.T
        for i in range(count):
            lq_out[divmod(i, nested) if nested else i] = jnp.broadcast_to(turned[:, 8 * i:8 * i + 1], (ROWS, ROWS))
            hi = turned[:, 8 * i + 1:8 * i + 2].astype(jnp.int32)
            lo = turned[:, 8 * i + 2:8 * i + 3].astype(jnp.int32)
            id_out[divmod(i, nested) if nested else i] = jnp.broadcast_to(hi * 65536 + lo, (ROWS, ROWS))
            row_hi = flat[8 * i + 1:8 * i + 2].astype(jnp.int32)
            row_lo = flat[8 * i + 2:8 * i + 3].astype(jnp.int32)
            id_row[:, i * ROWS:(i + 1) * ROWS] = row_hi * 65536 + row_lo

    meta_k.recv()
    columns(s.meta_small, s.lqc_small, s.idc_small, s.idr_small, n_small, 0)
    meta_z.recv()
    columns(s.meta_plane, s.lqc_plane, s.idc_plane, s.idr_plane, n_plane, ny)

    def transposed(value):
        return value.astype(F32).T.astype(BF16)

    for t in (0, 1):
        s.xt[t, k] = x_in[t][...].T.astype(BF16)
        s.h1t[t, k] = transposed(s.h1[t][...])
        s.h2t[t, k] = transposed(s.h2[t][...])
    saved = Exchange([(i, None, at_peer(AK, 1)) for i in range(3)])
    for i, ref in enumerate((s.xt, s.h1t, s.h2t)):
        saved.post(i, ref.at[1 - k, k], ref.at[1 - k, k])
    saved_end = len(started)

    v_own = s.small[1][k, x]
    u_own = s.small[0][k, x]
    eye = (lax.broadcasted_iota(jnp.int32, (ROWS, ROWS), 0) == lax.broadcasted_iota(jnp.int32, (ROWS, ROWS), 1))
    own_scores = mm(v_own, u_own, C11) * INV_TEMP - s.lqc_small[k * nx + x]
    s.pos[...] = jnp.sum(jnp.where(eye, own_scores, 0.0), axis=0, keepdims=True)

    u_small_k.recv()

    def twice(value):
        return jnp.concatenate([value, value], axis=1)

    def score_tile(slot, items, lq_part, id_part):
        s.plane_t[:, pl.ds(pl.multiple_of(slot * tile_rows, tile_rows), tile_rows)] = transposed(items)
        lq_wide = twice(lq_part.reshape(tile_rows, ROWS))
        id_wide = twice(id_part.reshape(tile_rows, ROWS))
        for n in range(n_chunk):
            lanes = slice(n * 256, (n + 1) * 256)
            queries = s.small[0][2 * n // nx, pl.ds(2 * n % nx, 2)].reshape(256, EMB)
            score = mm(items, queries, C11) * INV_TEMP - lq_wide
            score = jnp.where(id_wide == s.idr_small[:, lanes], -jnp.inf, score)
            peak = jnp.maximum(jnp.max(score, axis=0, keepdims=True), NEG)
            prob = jnp.exp(score - peak)
            s.probs[slot, :, lanes] = prob
            s.tile_max[slot, :, lanes] = peak
            s.tile_sum[slot, :, lanes] = jnp.sum(prob, axis=0, keepdims=True)

    def score_step(index, carry):
        turn = jnp.where(index == 2, 3, jnp.where(index == 3, 2, index))
        ref = s.plane[1]

        @pl.when(index > 0)
        def _():
            for part, view in zip(v_second, (ref.at[z, :, top], ref.at[:, y, low])):
                part.one(index - 1, view).wait_recv()

        iz = lax.rem(z - turn + nz, nz)
        iy = lax.rem(y - turn + ny, ny)
        score_tile(2 * index, ref[iz, :, top].reshape(tile_rows, EMB), s.lqc_plane[iz, :, top], s.idc_plane[iz, :, top])
        score_tile(2 * index + 1, ref[:, iy, low].reshape(tile_rows, EMB), s.lqc_plane[:, iy, low], s.idc_plane[:, iy, low])
        return carry

    lax.fori_loop(0, nz, score_step, 0)

    tile_max = s.tile_max[...]
    part_max = jnp.max(tile_max, axis=0)
    part_sum = jnp.sum(s.tile_sum[...] * jnp.exp(tile_max - part_max[None]), axis=0)
    for i in range(n_small):
        s.stats[k, x, i:i + 1] = part_max[:, i * ROWS:(i + 1) * ROWS]
        s.stats[k, x, n_small + i:n_small + i + 1] = part_sum[:, i * ROWS:(i + 1) * ROWS]
    own_block = k * nx + x
    pos = s.pos[...]
    old_max = s.stats[k, x, pl.ds(own_block, 1)]
    new_max = jnp.maximum(old_max, pos)
    s.stats[k, x, pl.ds(own_block, 1)] = new_max
    s.stats[k, x, pl.ds(n_small + own_block, 1)] = (
        s.stats[k, x, pl.ds(n_small + own_block, 1)] * jnp.exp(old_max - new_max) + jnp.exp(pos - new_max))
    stats_ref = s.stats.at[k, x]
    stats = small_group().send(lambda r, d: stats_ref, lambda r, d: stats_ref)

    v_small_k.recv()
    for part in u_second:
        part.recv()

    stages = ((2, 1), (3, 0)) if nx == 4 else ((1, 0),)

    n_wide_tile = n_wide // 256

    def wide_tile(chunk, carry):
        side = jnp.where(lax.rem(chunk, 2) == 0, 1 - k, k)
        spots = []
        for turns in zip(*stages):
            spots.append(lax.rem(x + jnp.where(chunk // 2 == 0, turns[0], turns[-1]), nx))
        items = jnp.concatenate([s.small[1][side, spot] for spot in spots], axis=0)
        lq_wide = twice(jnp.concatenate([s.lqc_small[side * nx + spot] for spot in spots], axis=0))
        id_wide = twice(jnp.concatenate([s.idc_small[side * nx + spot] for spot in spots], axis=0))
        for n in range(n_wide_tile):
            lanes = slice(n * 256, (n + 1) * 256)
            queries = s.plane[0][2 * n // ny, pl.ds(2 * n % ny, 2)].reshape(256, EMB)
            score = mm(items, queries, C11) * INV_TEMP - lq_wide
            s.scores[chunk, :, lanes] = jnp.where(id_wide == s.idr_plane[:, lanes], -jnp.inf, score)
        return carry

    lax.fori_loop(0, n_chunk, wide_tile, 0)

    stats.recv()
    every = s.stats[...].reshape(n_small, 2 * n_small, ROWS)
    all_max = jnp.max(every[:, :n_small], axis=0)
    all_sum = jnp.zeros_like(all_max)
    for i in range(n_small):
        all_sum = all_sum + every[i, n_small:] * jnp.exp(every[i, :n_small] - all_max)
    all_inv = 1.0 / (all_sum * batch)
    s.stat_all[:n_small] = all_max
    s.stat_all[n_small:] = all_sum
    for i in range(n_small):
        s.row_max[:, i * ROWS:(i + 1) * ROWS] = all_max[i:i + 1]
        s.row_inv[:, i * ROWS:(i + 1) * ROWS] = all_inv[i:i + 1]
    own_max = s.stat_all[pl.ds(own_block, 1)]
    own_sum = s.stat_all[pl.ds(n_small + own_block, 1)]
    s.ml[z, y] = jnp.concatenate([own_max, own_sum, pos] + [zero_row] * 5, axis=0)
    ml_ref = s.ml.at[z, y]
    ml_plane = plane_group().send(lambda r, d: ml_ref, lambda r, d: ml_ref)
    own_grad = (jnp.exp(pos - own_max) / own_sum - 1.0) / batch
    s.own_diag[...] = jnp.where(eye, jnp.broadcast_to(own_grad, (ROWS, ROWS)), 0.0).astype(BF16)

    s.factor[...] = (jnp.exp(tile_max - s.row_max[:, :n_query][None]) * s.row_inv[:, :n_query][None])

    def user_chunk(index, carry):
        chunk = lax.rem((1 - k) * (n_chunk // 2) + index, n_chunk)
        lanes = pl.ds(pl.multiple_of(chunk * 256, 256), 256)
        for tile in range(n_tile):
            s.grad_tile[tile * tile_rows:(tile + 1) * tile_rows] = (
                s.probs[tile, :, lanes] * s.factor[tile, :, lanes]).astype(BF16)
        turned = mm(s.plane_t[...], s.grad_tile[...])
        s.parts[0][2 * chunk] = turned[:, :ROWS]
        s.parts[0][2 * chunk + 1] = turned[:, ROWS:]
        return carry

    def to_partner(t):
        ref = s.parts[t]
        into = s.from_core[t]
        return along(AK).send(lambda r, d: ref.at[pl.ds((1 - k) * nx, nx)], lambda r, d: into)

    def to_x(t, exchange):
        exchange.recv()
        for i in range(nx):
            s.core_sum[t][i] = s.parts[t][k * nx + i] + s.from_core[t][i]
        return along(AX).send(lambda r, d: s.core_sum[t].at[d], lambda r, d: s.from_x[t].at[r - 1])

    def summed(t, exchange):
        exchange.recv()
        total = s.core_sum[t][x]
        for r in range(1, nx):
            total = total + s.from_x[t][r - 1]
        return total * INV_TEMP

    lax.fori_loop(0, n_chunk // 2, user_chunk, 0)
    du_core = to_partner(0)
    lax.fori_loop(n_chunk // 2, n_chunk, user_chunk, 0)
    s.parts[0][own_block] = s.parts[0][own_block] + mm(v_own, s.own_diag[...], C00)
    du_x = to_x(0, du_core)
    drain(saved_end)
    ml_plane.recv()
    loss_row = jnp.zeros((1, ROWS), F32)
    for iz in range(nz):
        for iy in range(ny):
            i = iz * ny + iy
            row = s.ml[iz, iy]
            s.row_max[:, i * ROWS:(i + 1) * ROWS] = row[0:1]
            s.row_inv[:, i * ROWS:(i + 1) * ROWS] = 1.0 / (row[1:2] * batch)
            loss_row = loss_row + ((row[0:1] - row[2:3]) + jnp.log(row[1:2]))
    s.lx[k, x] = jnp.broadcast_to(loss_row, (8, ROWS))
    lx_ref = s.lx.at[k, x]
    loss_x = small_group().send(lambda r, d: lx_ref, lambda r, d: lx_ref)

    def item_chunk(stage, side, own):
        chunk = 2 * stage + own
        grads = []
        for n in range(n_wide_tile):
            lanes = slice(n * 256, (n + 1) * 256)
            grads.append((jnp.exp(s.scores[chunk, :, lanes] - s.row_max[:, lanes])
                          * s.row_inv[:, lanes]).astype(BF16))
        total = mm(jnp.concatenate(grads, axis=1), s.plane[0][...].reshape(n_wide, EMB))
        for i, r in enumerate(stages[stage]):
            s.parts[1][side * nx + wrap(AX, r)] = total[i * ROWS:(i + 1) * ROWS]

    dv_core = Exchange([(i, None, at_peer(AK, 1)) for i in range(nx)])
    dv_x = along(AX)
    for stage, turns in enumerate(stages):
        item_chunk(stage, 1 - k, 0)
        for i, r in enumerate(turns):
            spot = wrap(AX, r)
            dv_core.post(2 * stage + i, s.parts[1].at[(1 - k) * nx + spot], s.from_core[1].at[spot])
        item_chunk(stage, k, 1)
        if 0 in turns:
            s.parts[1][own_block] = s.parts[1][own_block] + mm(s.own_diag[...], u_own)
        for i, r in enumerate(turns):
            spot = wrap(AX, r)
            dv_core.copies[2 * stage + i].wait_recv()
            s.core_sum[1][spot] = s.parts[1][k * nx + spot] + s.from_core[1][spot]
            if r:
                dv_x.post(order(nx).index(r), s.core_sum[1].at[spot], s.from_x[1].at[r - 1])
    middle = len(started)

    def backward(t, grad_unit):
        unit = s.unit[t][...]
        grad_raw = s.inv[t][...] * (grad_unit - unit * jnp.sum(unit * grad_unit, axis=1, keepdims=True))
        grad_three = grad_raw.astype(BF16)
        s.g3[t, k] = grad_three
        back = mm(grad_three, s.wh[t][2][...], C11)
        grad_two = jnp.where(s.h2[t][...] > 0, back, 0.0).astype(BF16)
        s.g2[t, k] = grad_two
        back = mm(grad_two, s.wh[t][1][...], C11)
        s.g1[t, k] = jnp.where(s.h1[t][...] > 0, back, 0.0).astype(BF16)

    axes = ((AX, AY, AZ), (AY, AZ, AX), (AZ, AX, AY))
    own_rows = [[None, None] for _ in axes]
    for q, (first, second, _) in enumerate(axes):
        high = ROWS // size[first]
        step = high // size[second]
        own_rows[q][0] = pl.ds(pl.multiple_of(co[first] * high, high), high)
        own_rows[q][1] = pl.ds(pl.multiple_of(co[first] * high + co[second] * step, step), step)
    scatter_a = [along(axes[q][0]) for q in range(3)]

    def pair_copy(t, i):
        ref = (s.g3, s.g2, s.g1)[i].at[t, 1 - t]
        index = grad_pair.base + 3 * t + i
        return pltpu.make_async_remote_copy(
            src_ref=ref, dst_ref=ref, send_sem=s.send_sem.at[index], recv_sem=s.recv_sem.at[index],
            device_id=(grad_pair.peers[0][2],), device_id_type=MESH)

    grad_pair = Exchange([(i, None, at_peer(AK, 1)) for i in range(6)])

    def hand_grads(t):
        @pl.when(k != t)
        def _():
            for i in range(3):
                pair_copy(t, i).start()

    def weight_grads(t):
        @pl.when(k == t)
        def _():
            def rows(ref, depth):
                return jnp.concatenate([ref[t, i] for i in range(nk)], axis=1)

            pair_copy(t, 0).wait_recv()
            third = mm(rows(s.h2t, WIDE), s.g3[t].reshape(nk * ROWS, EMB))
            for i in range(3):
                s.dw[2, 1, :, i * EMB:(i + 1) * EMB] = third[i * ROWS:(i + 1) * ROWS]
            pair_copy(t, 1).wait_recv()
            second = mm(rows(s.h1t, WIDE), s.g2[t].reshape(nk * ROWS, WIDE))
            s.dw[1, 0] = second[:ROWS]
            s.dw[1, 1] = second[ROWS:2 * ROWS]
            s.dw[2, 0] = second[2 * ROWS:]
            start_scatter(2)
            start_scatter(1)
            pair_copy(t, 2).wait_recv()
            first = mm(rows(s.xt, IN_WIDTH), s.g1[t].reshape(nk * ROWS, WIDE))
            s.dw[0, 0] = first[:ROWS]
            s.dw[0, 1] = first[ROWS:]
            start_scatter(0)

    def scatter_copy(q, i):
        high = ROWS // size[axes[q][0]]
        r, dest, dev = scatter_a[q].peers[i]
        index = scatter_a[q].base + i
        return pltpu.make_async_remote_copy(
            src_ref=s.dw.at[q, :, pl.ds(pl.multiple_of(dest * high, high), high)], dst_ref=s.ra[q].at[r - 1],
            send_sem=s.send_sem.at[index], recv_sem=s.recv_sem.at[index],
            device_id=(dev,), device_id_type=MESH)

    def start_scatter(q):
        for i in range(len(scatter_a[q].peers)):
            scatter_copy(q, i).start()

    grad_user = summed(0, du_x).T
    backward(0, grad_user)
    hand_grads(0)
    saved.recv()
    weight_grads(0)
    drain(middle)
    grad_item = summed(1, dv_x)
    backward(1, grad_item)
    hand_grads(1)
    weight_grads(1)
    order_q = (2, 1, 0)
    scatter_b = {}
    for q in order_q:
        for i in range(len(scatter_a[q].peers)):
            scatter_copy(q, i).wait_recv()
        first, second, _ = axes[q]
        value = s.dw[q, :, own_rows[q][0]]
        for r in range(size[first] - 1):
            value = value + s.ra[q][r]
        s.sa[q][...] = value
        step = ROWS // size[first] // size[second]
        scatter_b[q] = along(second).send(
            lambda r, d, q=q, step=step: s.sa[q].at[:, pl.ds(pl.multiple_of(d * step, step), step)],
            lambda r, d, q=q: s.rb[q].at[r - 1])
    for q in order_q:
        for i in range(len(scatter_a[q].peers)):
            scatter_copy(q, i).wait_send()
    for t in range(2):
        @pl.when(k != t)
        def _():
            for i in range(3):
                pair_copy(t, i).wait_send()
    second_end = len(started)
    exchange_c = {}
    for q in order_q:
        scatter_b[q].recv()
        first, second, third = axes[q]
        step = ROWS // size[first] // size[second]
        value = s.sa[q][:, pl.ds(pl.multiple_of(co[second] * step, step), step)]
        for r in range(size[second] - 1):
            value = value + s.rb[q][r]
        s.cx[q][co[third]] = value
        exchange_c[q] = share(third, s.cx[q].at[co[third]])
    drain(second_end)
    third_end = len(started)
    gather_b = {}
    for q in order_q:
        exchange_c[q].recv()
        value = s.cx[q][0]
        for r in range(1, size[axes[q][2]]):
            value = value + s.cx[q][r]
        out_ref[k, q, :, own_rows[q][1]] = value
        gather_b[q] = share(axes[q][1], out_ref.at[k, q, :, own_rows[q][1]])
    drain(third_end)
    loss_x.recv()
    loss_total = jnp.zeros((8, ROWS), F32)
    for ik in range(nk):
        for ix in range(nx):
            loss_total = loss_total + s.lx[ik, ix]
    loss_ref[...] = loss_total
    fourth_end = len(started)
    gather_a = {}
    handed = []
    for q in order_q:
        gather_b[q].recv()
        gather_a[q] = share(axes[q][0], out_ref.at[k, q, :, own_rows[q][0]])
    for q in order_q:
        handed.append(share(AK, out_ref.at[k, q, :, own_rows[q][0]]))
    drain(fourth_end)
    for i in range(max(size) - 1):
        for q in order_q:
            first = axes[q][0]
            high = ROWS // size[first]
            r = gather_a[q].peers[i][0]
            gather_a[q].copies[i].wait_recv()
            source = lax.rem(co[first] - r + size[first], size[first])
            handed.append(share(AK, out_ref.at[k, q, :, pl.ds(pl.multiple_of(source * high, high), high)]))
    for exchange in handed:
        exchange.recv()
    drain(len(started))


def finish_kernel(batch, res_ref, loss_in, loss_ref, *outs):
    loss_ref[...] = jnp.sum(loss_in[0:1], axis=1, keepdims=True) / batch
    for t in range(2):
        one, two, three = outs[3 * t:3 * t + 3]
        for i in range(2):
            one[i * ROWS:(i + 1) * ROWS] = res_ref[t, 0, i]
        for i in range(3):
            two[i * ROWS:(i + 1) * ROWS] = res_ref[t, 1 + i // 2, i % 2]
            three[i * ROWS:(i + 1) * ROWS] = res_ref[t, 2, 1, :, i * EMB:(i + 1) * EMB]


def solution(mesh):
    devices = mesh.shape['dp']
    grid = GRIDS[devices]
    scratch, tree = jax.tree.flatten(scratch_table(*grid))
    vmem = pl.BlockSpec(memory_space=pltpu.VMEM)

    def device_step(user_x, item_x, item_id, log_q, user_w1, user_w2, user_w3, item_w1, item_w2, item_w3):
        res, loss_rows = pl.pallas_call(
            functools.partial(step_kernel, grid, tree),
            out_shape=(jax.ShapeDtypeStruct((2, 3, 2, ROWS, WIDE), F32), jax.ShapeDtypeStruct((8, ROWS), F32)),
            in_specs=[vmem] * 10,
            out_specs=(vmem, vmem),
            scratch_shapes=scratch,
            compiler_params=pltpu.CompilerParams(collective_id=0, has_side_effects=True, vmem_limit_bytes=40 * 1024 * 1024),
            name='train_step',
        )(user_x, item_x, log_q.reshape(1, ROWS), item_id.reshape(1, ROWS), user_w1, user_w2, user_w3, item_w1, item_w2, item_w3)
        shapes = [(IN_WIDTH, WIDE), (WIDE, WIDE), (WIDE, EMB)] * 2
        outs = pl.pallas_call(
            functools.partial(finish_kernel, float(devices * ROWS)),
            out_shape=[jax.ShapeDtypeStruct((1, 1), F32)] + [jax.ShapeDtypeStruct(shape, F32) for shape in shapes],
            in_specs=[vmem, vmem],
            out_specs=[vmem] * 7,
            compiler_params=pltpu.CompilerParams(vmem_limit_bytes=12 * 1024 * 1024),
            name='finish',
        )(res, loss_rows)
        return (outs[0].reshape(()),) + tuple(outs[1:])

    rows, vec, whole = P('dp', None), P('dp'), P()
    return jax.shard_map(device_step, mesh=mesh, in_specs=(rows, rows, vec, vec) + (whole,) * 6,
                         out_specs=(whole,) * 7, check_vma=False)
```

```python
import functools

import jax
import jax.numpy as jnp
from jax import lax
from jax.experimental import pallas as pl
from jax.experimental.pallas import tpu as pltpu
from jax.sharding import PartitionSpec as P

MESH = pl.DeviceIdType.MESH
F32 = jnp.float32
BF16 = jnp.bfloat16
INV_TEMP = 1.0 / 0.05
NORM_EPS = 1e-6
ROWS = 128
EMB = 128
WIDE = 384
IN_WIDTH = 256
NEG = -3.0e38
GRIDS = {128: (4, 4, 4, 2), 16: (2, 2, 2, 2)}
AZ, AY, AX, AK = range(4)
C00 = (((0,), (0,)), ((), ()))
C11 = (((1,), (1,)), ((), ()))
C10 = (((1,), (0,)), ((), ()))
N_REMOTE = 192


def mm(a, b, dims=C10):
    return lax.dot_general(a, b, dims, preferred_element_type=F32)


def scratch_table(nz, ny, nx, nk):
    n_plane, n_small = nz * ny, nk * nx
    n_tile, tile_rows = nz + ny, ny * ROWS // 2
    n_query = n_small * ROWS
    n_wide = n_plane * ROWS
    longest = max(n_wide, n_query)
    turns = ((nx, ny, nz), (ny, nz, nx), (nz, nx, ny))

    def vm(dtype, *shape):
        return pltpu.VMEM(shape, dtype)

    def two(dtype, *shape):
        return [vm(dtype, *shape) for _ in range(2)]

    def each(shape_of):
        return [vm(F32, *shape_of(*turn), WIDE) for turn in turns]

    return dict(
        wh=[[vm(BF16, IN_WIDTH, WIDE), vm(BF16, WIDE, WIDE), vm(BF16, WIDE, EMB)] for _ in range(2)],
        xf=two(F32, ROWS, IN_WIDTH),
        wf=[[vm(F32, IN_WIDTH, WIDE), vm(F32, WIDE, WIDE), vm(F32, WIDE, EMB)] for _ in range(2)],
        lq=vm(F32, 1, ROWS),
        ids=vm(jnp.int32, 1, ROWS),
        h1=two(BF16, ROWS, WIDE),
        h2=two(BF16, ROWS, WIDE),
        xt=vm(BF16, 2, nk, IN_WIDTH, ROWS),
        h1t=vm(BF16, 2, nk, WIDE, ROWS),
        h2t=vm(BF16, 2, nk, WIDE, ROWS),
        g1=vm(BF16, 2, nk, ROWS, WIDE),
        g2=vm(BF16, 2, nk, ROWS, WIDE),
        g3=vm(BF16, 2, nk, ROWS, EMB),
        unit=two(F32, ROWS, EMB),
        inv=two(F32, ROWS, EMB),
        plane=two(BF16, nz, ny, ROWS, EMB),
        small=two(BF16, nk, nx, ROWS, EMB),
        parts=two(F32, n_small, ROWS, EMB),
        from_core=two(F32, nx, ROWS, EMB),
        core_sum=two(F32, nx, ROWS, EMB),
        from_x=two(F32, nx - 1, ROWS, EMB),
        dw=vm(F32, 3, 2, ROWS, WIDE),
        ra=each(lambda a, b, c: (a - 1, 2, ROWS // a)),
        sa=each(lambda a, b, c: (2, ROWS // a)),
        rb=each(lambda a, b, c: (b - 1, 2, ROWS // a // b)),
        cx=each(lambda a, b, c: (c, 2, ROWS // a // b)),
        meta_plane=vm(F32, nz, ny, 8, ROWS),
        meta_small=vm(F32, nk, nx, 8, ROWS),
        lqc_plane=vm(F32, nz, ny, ROWS, ROWS),
        idc_plane=vm(jnp.int32, nz, ny, ROWS, ROWS),
        lqc_small=vm(F32, n_small, ROWS, ROWS),
        idc_small=vm(jnp.int32, n_small, ROWS, ROWS),
        idr_plane=vm(jnp.int32, 1, n_wide),
        idr_small=vm(jnp.int32, 1, n_query),
        probs=vm(F32, n_tile, tile_rows, n_query),
        tile_max=vm(F32, n_tile, 1, n_query),
        tile_sum=vm(F32, n_tile, 1, n_query),
        factor=vm(F32, n_tile, 1, n_query),
        stats=vm(F32, nk, nx, 2 * n_small, ROWS),
        stat_all=vm(F32, 2 * n_small, ROWS),
        plane_t=vm(BF16, EMB, n_wide),
        grad_tile=vm(BF16, n_wide, 256),
        scores=vm(F32, n_small // 2, 256, n_wide),
        chunk_max=vm(F32, n_small // 2, 1, n_wide),
        row_max=vm(F32, 1, longest),
        row_inv=vm(F32, 1, longest),
        ml=vm(F32, nz, ny, 8, ROWS),
        lx=vm(F32, nk, nx, 8, ROWS),
        own_diag=vm(BF16, ROWS, ROWS),
        pos=vm(F32, 1, ROWS),
        send_sem=pltpu.SemaphoreType.DMA((N_REMOTE,)),
        recv_sem=pltpu.SemaphoreType.DMA((N_REMOTE,)),
        load_sem=pltpu.SemaphoreType.DMA((10,)),
    )


class Space:
    def __init__(self, entries):
        self.__dict__.update(entries)


def step_kernel(grid, tree, *refs):
    nz, ny, nx, nk = grid
    n_plane, n_small = nz * ny, nk * nx
    n_tile, tile_rows = nz + ny, ny * ROWS // 2
    n_chunk = n_small // 2
    n_query = n_small * ROWS
    n_wide = n_plane * ROWS
    batch = float(nz * ny * nx * nk * ROWS)
    x_in, lq_in, id_in = refs[0:2], refs[2], refs[3]
    w_in = (refs[4:7], refs[7:10])
    out_ref, loss_ref = refs[10:12]
    s = Space(jax.tree.unflatten(tree, refs[12:]))

    me = lax.axis_index('dp')
    size = grid
    stride = (ny * nx * nk, nx * nk, nk, 1)
    co = tuple(lax.rem(me // stride[ax], size[ax]) for ax in range(4))
    z, y, x, k = co

    def wrap(ax, r):
        return lax.rem(co[ax] + r, size[ax])

    def at_peer(ax, r):
        return me + (wrap(ax, r) - co[ax]) * stride[ax]

    def order(n):
        return sorted(range(1, n), key=lambda r: min(r, n - r))

    used = [0]
    started = []
    drained = [0]

    class Exchange:
        def __init__(self, peers):
            self.peers = peers
            self.base = used[0]
            used[0] += len(peers)
            self.copies = {}

        def post(self, index, src, dst):
            copy = pltpu.make_async_remote_copy(
                src_ref=src, dst_ref=dst,
                send_sem=s.send_sem.at[self.base + index], recv_sem=s.recv_sem.at[self.base + index],
                device_id=(self.peers[index][2],), device_id_type=MESH)
            copy.start()
            self.copies[index] = copy
            started.append(copy)

        def send(self, src, dst):
            for i, (r, dest, dev) in enumerate(self.peers):
                self.post(i, src(r, dest), dst(r, dest))
            return self

        def recv(self):
            for copy in self.copies.values():
                copy.wait_recv()

        def one(self, index, view):
            return pltpu.make_async_remote_copy(
                src_ref=view, dst_ref=view,
                send_sem=s.send_sem.at[self.base + index], recv_sem=s.recv_sem.at[self.base + index],
                device_id=(self.peers[0][2],), device_id_type=MESH)

    def along(ax):
        return Exchange([(r, wrap(ax, r), at_peer(ax, r)) for r in order(size[ax])])

    def share(ax, ref):
        return along(ax).send(lambda r, d: ref, lambda r, d: ref)

    def small_group():
        peers = []
        for rk in range(nk):
            for rx in [0] + order(nx):
                if rk or rx:
                    dev = me + (wrap(AK, rk) - k) + (wrap(AX, rx) - x) * nk
                    peers.append((len(peers), None, dev))
        return Exchange(peers)

    def plane_group():
        peers = []
        for rz in [0] + order(nz):
            for ry in [0] + order(ny):
                if rz or ry:
                    peers.append((len(peers), None, me + (wrap(AZ, rz) - z) * stride[AZ] + (wrap(AY, ry) - y) * stride[AY]))
        return Exchange(peers)

    def drain(upto):
        while drained[0] < upto:
            started[drained[0]].wait_send()
            drained[0] += 1

    loads = []

    def load(src, dst):
        copy = pltpu.make_async_copy(src, dst, s.load_sem.at[len(loads)])
        copy.start()
        loads.append(copy)
        return copy

    load_x, load_w = {}, {}
    for t in (1, 0):
        load_x[t] = load(x_in[t], s.xf[t])
        load_w[t] = [load(w_in[t][i], s.wf[t][i]) for i in range(3)]
        if t:
            load_meta = load(lq_in, s.lq), load(id_in, s.ids)

    barrier = pltpu.get_barrier_semaphore()
    greet = [at_peer(ax, r) for ax in (AZ, AY, AX, AK) for r in range(1, size[ax])]
    greet += [me + (wrap(AK, rk) - k) + (wrap(AX, rx) - x) * nk for rk in range(1, nk) for rx in range(1, nx)]
    greet += [me + (wrap(AZ, rz) - z) * stride[AZ] + (wrap(AY, ry) - y) * stride[AY] for rz in range(1, nz) for ry in range(1, ny)]
    for dev in greet:
        pl.semaphore_signal(barrier, inc=1, device_id=(dev,), device_id_type=MESH)

    def forward(t):
        load_x[t].wait()
        xb = s.xf[t][...].astype(BF16)
        for i in range(3):
            load_w[t][i].wait()
            s.wh[t][i][...] = s.wf[t][i][...].astype(BF16)
        act = jnp.maximum(mm(xb, s.wh[t][0][...]), 0.0).astype(BF16)
        s.h1[t][...] = act
        act = jnp.maximum(mm(act, s.wh[t][1][...]), 0.0).astype(BF16)
        s.h2[t][...] = act
        raw = mm(act, s.wh[t][2][...])
        inv = lax.rsqrt(jnp.sum(raw * raw, axis=1, keepdims=True) + NORM_EPS)
        unit = raw * inv
        s.unit[t][...] = unit
        s.inv[t][...] = jnp.broadcast_to(inv, (ROWS, EMB))
        half = unit.astype(BF16)
        s.plane[t][z, y] = half
        s.small[t][k, x] = half

    half_rows = ROWS // 2
    top, low = pl.ds(0, half_rows), pl.ds(half_rows, half_rows)

    def plane_first(t):
        ref = s.plane[t]
        return share(AY, ref.at[z, y, top]), share(AZ, ref.at[z, y, low])

    def plane_second(t, first):
        ref = s.plane[t]
        first[0].recv()
        a = share(AZ, ref.at[z, :, top])
        first[1].recv()
        b = share(AY, ref.at[:, y, low])
        return a, b

    forward(1)
    for copy in load_meta:
        copy.wait()
    ids = s.ids[...]
    zero_row = jnp.zeros((1, ROWS), F32)
    meta = jnp.concatenate([s.lq[...], lax.shift_right_logical(ids, 16).astype(F32),
                            lax.bitwise_and(ids, 65535).astype(F32)] + [zero_row] * 5, axis=0)
    s.meta_plane[z, y] = meta
    s.meta_small[k, x] = meta
    pl.semaphore_wait(barrier, len(greet))
    meta_y = share(AY, s.meta_plane.at[z, y])
    meta_x = share(AX, s.meta_small.at[k, x])
    v_first = plane_first(1)
    v_small = share(AX, s.small[1].at[k, x])
    forward(0)
    u_small = share(AX, s.small[0].at[k, x])
    u_first = plane_first(0)
    meta_y.recv()
    meta_z = share(AZ, s.meta_plane.at[z])
    meta_x.recv()
    meta_k = share(AK, s.meta_small.at[k])
    v_second = plane_second(1, v_first)
    def columns(ref, lq_out, id_out, id_row, count, nested):
        flat = ref[...].reshape(count * 8, ROWS)
        if count * 8 < ROWS:
            flat = jnp.concatenate([flat, jnp.zeros((ROWS - count * 8, ROWS), F32)], axis=0)
        turned = flat.T
        for i in range(count):
            lq_out[divmod(i, nested) if nested else i] = jnp.broadcast_to(turned[:, 8 * i:8 * i + 1], (ROWS, ROWS))
            hi = turned[:, 8 * i + 1:8 * i + 2].astype(jnp.int32)
            lo = turned[:, 8 * i + 2:8 * i + 3].astype(jnp.int32)
            id_out[divmod(i, nested) if nested else i] = jnp.broadcast_to(hi * 65536 + lo, (ROWS, ROWS))
            row_hi = flat[8 * i + 1:8 * i + 2].astype(jnp.int32)
            row_lo = flat[8 * i + 2:8 * i + 3].astype(jnp.int32)
            id_row[:, i * ROWS:(i + 1) * ROWS] = row_hi * 65536 + row_lo

    meta_k.recv()
    columns(s.meta_small, s.lqc_small, s.idc_small, s.idr_small, n_small, 0)
    meta_z.recv()
    columns(s.meta_plane, s.lqc_plane, s.idc_plane, s.idr_plane, n_plane, ny)

    def transposed(value):
        return value.astype(F32).T.astype(BF16)

    u_small.recv()
    u_small_k = share(AK, s.small[0].at[k])
    u_second = plane_second(0, u_first)
    v_small.recv()
    v_small_k = share(AK, s.small[1].at[k])

    for t in (0, 1):
        s.xt[t, k] = s.xf[t][...].T.astype(BF16)
        s.h1t[t, k] = transposed(s.h1[t][...])
        s.h2t[t, k] = transposed(s.h2[t][...])
    saved = Exchange([(i, None, at_peer(AK, 1)) for i in range(3)])
    for i, ref in enumerate((s.xt, s.h1t, s.h2t)):
        saved.post(i, ref.at[1 - k, k], ref.at[1 - k, k])
    saved_end = len(started)

    v_own = s.small[1][k, x]
    u_own = s.small[0][k, x]
    eye = (lax.broadcasted_iota(jnp.int32, (ROWS, ROWS), 0) == lax.broadcasted_iota(jnp.int32, (ROWS, ROWS), 1))
    own_scores = mm(v_own, u_own, C11) * INV_TEMP - s.lqc_small[k * nx + x]
    s.pos[...] = jnp.sum(jnp.where(eye, own_scores, 0.0), axis=0, keepdims=True)

    u_small_k.recv()

    def twice(value):
        return jnp.concatenate([value, value], axis=1)

    def score_tile(slot, items, lq_part, id_part):
        s.plane_t[:, pl.ds(pl.multiple_of(slot * tile_rows, tile_rows), tile_rows)] = transposed(items)
        lq_wide = twice(lq_part.reshape(tile_rows, ROWS))
        id_wide = twice(id_part.reshape(tile_rows, ROWS))
        for n in range(n_chunk):
            lanes = slice(n * 256, (n + 1) * 256)
            queries = s.small[0][2 * n // nx, pl.ds(2 * n % nx, 2)].reshape(256, EMB)
            score = mm(items, queries, C11) * INV_TEMP - lq_wide
            score = jnp.where(id_wide == s.idr_small[:, lanes], -jnp.inf, score)
            peak = jnp.maximum(jnp.max(score, axis=0, keepdims=True), NEG)
            prob = jnp.exp(score - peak)
            s.probs[slot, :, lanes] = prob
            s.tile_max[slot, :, lanes] = peak
            s.tile_sum[slot, :, lanes] = jnp.sum(prob, axis=0, keepdims=True)

    def score_step(index, carry):
        turn = jnp.where(index == 2, 3, jnp.where(index == 3, 2, index))
        ref = s.plane[1]

        @pl.when(index > 0)
        def _():
            for part, view in zip(v_second, (ref.at[z, :, top], ref.at[:, y, low])):
                part.one(index - 1, view).wait_recv()

        iz = lax.rem(z - turn + nz, nz)
        iy = lax.rem(y - turn + ny, ny)
        score_tile(2 * index, ref[iz, :, top].reshape(tile_rows, EMB), s.lqc_plane[iz, :, top], s.idc_plane[iz, :, top])
        score_tile(2 * index + 1, ref[:, iy, low].reshape(tile_rows, EMB), s.lqc_plane[:, iy, low], s.idc_plane[:, iy, low])
        return carry

    lax.fori_loop(0, nz, score_step, 0)

    tile_max = s.tile_max[...]
    part_max = jnp.max(tile_max, axis=0)
    part_sum = jnp.sum(s.tile_sum[...] * jnp.exp(tile_max - part_max[None]), axis=0)
    for i in range(n_small):
        s.stats[k, x, i:i + 1] = part_max[:, i * ROWS:(i + 1) * ROWS]
        s.stats[k, x, n_small + i:n_small + i + 1] = part_sum[:, i * ROWS:(i + 1) * ROWS]
    own_block = k * nx + x
    pos = s.pos[...]
    old_max = s.stats[k, x, pl.ds(own_block, 1)]
    new_max = jnp.maximum(old_max, pos)
    s.stats[k, x, pl.ds(own_block, 1)] = new_max
    s.stats[k, x, pl.ds(n_small + own_block, 1)] = (
        s.stats[k, x, pl.ds(n_small + own_block, 1)] * jnp.exp(old_max - new_max) + jnp.exp(pos - new_max))
    stats_ref = s.stats.at[k, x]
    stats = small_group().send(lambda r, d: stats_ref, lambda r, d: stats_ref)

    v_small_k.recv()
    for part in u_second:
        part.recv()

    stages = ((2, 1), (3, 0)) if nx == 4 else ((1, 0),)

    n_wide_tile = n_wide // 256

    def wide_tile(chunk, carry):
        side = jnp.where(lax.rem(chunk, 2) == 0, 1 - k, k)
        spots = []
        for turns in zip(*stages):
            spots.append(lax.rem(x + jnp.where(chunk // 2 == 0, turns[0], turns[-1]), nx))
        items = jnp.concatenate([s.small[1][side, spot] for spot in spots], axis=0)
        lq_wide = twice(jnp.concatenate([s.lqc_small[side * nx + spot] for spot in spots], axis=0))
        id_wide = twice(jnp.concatenate([s.idc_small[side * nx + spot] for spot in spots], axis=0))
        for n in range(n_wide_tile):
            lanes = slice(n * 256, (n + 1) * 256)
            queries = s.plane[0][2 * n // ny, pl.ds(2 * n % ny, 2)].reshape(256, EMB)
            score = mm(items, queries, C11) * INV_TEMP - lq_wide
            score = jnp.where(id_wide == s.idr_plane[:, lanes], -jnp.inf, score)
            peak = jnp.maximum(jnp.max(score, axis=0, keepdims=True), NEG)
            s.scores[chunk, :, lanes] = jnp.exp(score - peak)
            s.chunk_max[chunk, :, lanes] = peak
        return carry

    lax.fori_loop(0, 3 * n_chunk // 4, wide_tile, 0)

    stats.recv()
    every = s.stats[...].reshape(n_small, 2 * n_small, ROWS)
    all_max = jnp.max(every[:, :n_small], axis=0)
    all_sum = jnp.zeros_like(all_max)
    for i in range(n_small):
        all_sum = all_sum + every[i, n_small:] * jnp.exp(every[i, :n_small] - all_max)
    all_inv = 1.0 / (all_sum * batch)
    s.stat_all[:n_small] = all_max
    s.stat_all[n_small:] = all_sum
    for i in range(n_small):
        s.row_max[:, i * ROWS:(i + 1) * ROWS] = all_max[i:i + 1]
        s.row_inv[:, i * ROWS:(i + 1) * ROWS] = all_inv[i:i + 1]
    own_max = s.stat_all[pl.ds(own_block, 1)]
    own_sum = s.stat_all[pl.ds(n_small + own_block, 1)]
    s.ml[z, y] = jnp.concatenate([own_max, own_sum, pos] + [zero_row] * 5, axis=0)
    ml_ref = s.ml.at[z, y, pl.ds(0, 3)]
    ml_plane = plane_group().send(lambda r, d: ml_ref, lambda r, d: ml_ref)
    own_grad = (jnp.exp(pos - own_max) / own_sum - 1.0) / batch
    s.own_diag[...] = jnp.where(eye, jnp.broadcast_to(own_grad, (ROWS, ROWS)), 0.0).astype(BF16)

    s.factor[...] = (jnp.exp(tile_max - s.row_max[:, :n_query][None]) * s.row_inv[:, :n_query][None])

    def user_chunk(index, carry):
        chunk = lax.rem((1 - k) * (n_chunk // 2) + index, n_chunk)
        lanes = pl.ds(pl.multiple_of(chunk * 256, 256), 256)
        for tile in range(n_tile):
            s.grad_tile[tile * tile_rows:(tile + 1) * tile_rows] = (
                s.probs[tile, :, lanes] * s.factor[tile, :, lanes]).astype(BF16)
        turned = mm(s.plane_t[...], s.grad_tile[...])
        s.parts[0][2 * chunk] = turned[:, :ROWS]
        s.parts[0][2 * chunk + 1] = turned[:, ROWS:]
        return carry

    def to_partner(t):
        ref = s.parts[t]
        into = s.from_core[t]
        return along(AK).send(lambda r, d: ref.at[pl.ds((1 - k) * nx, nx)], lambda r, d: into)

    def to_x(t, exchange):
        exchange.recv()
        for i in range(nx):
            s.core_sum[t][i] = s.parts[t][k * nx + i] + s.from_core[t][i]
        return along(AX).send(lambda r, d: s.core_sum[t].at[d], lambda r, d: s.from_x[t].at[r - 1])

    def summed(t, exchange):
        exchange.recv()
        total = s.core_sum[t][x]
        for r in range(1, nx):
            total = total + s.from_x[t][r - 1]
        return total * INV_TEMP

    lax.fori_loop(0, n_chunk // 2, user_chunk, 0)
    du_core = to_partner(0)
    lax.fori_loop(n_chunk // 2, n_chunk, user_chunk, 0)
    s.parts[0][own_block] = s.parts[0][own_block] + mm(v_own, s.own_diag[...], C00)
    du_x = to_x(0, du_core)
    drain(saved_end)
    lax.fori_loop(3 * n_chunk // 4, n_chunk, wide_tile, 0)
    ml_plane.recv()
    loss_row = jnp.zeros((1, ROWS), F32)
    for iz in range(nz):
        for iy in range(ny):
            i = iz * ny + iy
            row = s.ml[iz, iy]
            s.row_max[:, i * ROWS:(i + 1) * ROWS] = row[0:1]
            s.row_inv[:, i * ROWS:(i + 1) * ROWS] = 1.0 / (row[1:2] * batch)
            loss_row = loss_row + ((row[0:1] - row[2:3]) + jnp.log(row[1:2]))
    s.lx[k, x] = jnp.broadcast_to(loss_row, (8, ROWS))
    lx_ref = s.lx.at[k, x]
    loss_x = small_group().send(lambda r, d: lx_ref, lambda r, d: lx_ref)

    def item_chunk(stage, side, own):
        chunk = 2 * stage + own
        grads = []
        for n in range(n_wide_tile):
            lanes = slice(n * 256, (n + 1) * 256)
            factor = jnp.exp(s.chunk_max[chunk, :, lanes] - s.row_max[:, lanes]) * s.row_inv[:, lanes]
            grads.append((s.scores[chunk, :, lanes] * factor).astype(BF16))
        total = mm(jnp.concatenate(grads, axis=1), s.plane[0][...].reshape(n_wide, EMB))
        for i, r in enumerate(stages[stage]):
            s.parts[1][side * nx + wrap(AX, r)] = total[i * ROWS:(i + 1) * ROWS]

    dv_core = Exchange([(i, None, at_peer(AK, 1)) for i in range(nx)])
    dv_x = along(AX)
    for stage, turns in enumerate(stages):
        item_chunk(stage, 1 - k, 0)
        for i, r in enumerate(turns):
            spot = wrap(AX, r)
            dv_core.post(2 * stage + i, s.parts[1].at[(1 - k) * nx + spot], s.from_core[1].at[spot])
        item_chunk(stage, k, 1)
        if 0 in turns:
            s.parts[1][own_block] = s.parts[1][own_block] + mm(s.own_diag[...], u_own)
        for i, r in enumerate(turns):
            spot = wrap(AX, r)
            dv_core.copies[2 * stage + i].wait_recv()
            s.core_sum[1][spot] = s.parts[1][k * nx + spot] + s.from_core[1][spot]
            if r:
                dv_x.post(order(nx).index(r), s.core_sum[1].at[spot], s.from_x[1].at[r - 1])
    middle = len(started)

    def backward(t, grad_unit):
        unit = s.unit[t][...]
        grad_raw = s.inv[t][...] * (grad_unit - unit * jnp.sum(unit * grad_unit, axis=1, keepdims=True))
        grad_three = grad_raw.astype(BF16)
        s.g3[t, k] = grad_three
        back = mm(grad_three, s.wh[t][2][...], C11)
        grad_two = jnp.where(s.h2[t][...] > 0, back, 0.0).astype(BF16)
        s.g2[t, k] = grad_two
        back = mm(grad_two, s.wh[t][1][...], C11)
        s.g1[t, k] = jnp.where(s.h1[t][...] > 0, back, 0.0).astype(BF16)

    axes = ((AX, AY, AZ), (AY, AZ, AX), (AZ, AX, AY))
    own_rows = [[None, None] for _ in axes]
    for q, (first, second, _) in enumerate(axes):
        high = ROWS // size[first]
        step = high // size[second]
        own_rows[q][0] = pl.ds(pl.multiple_of(co[first] * high, high), high)
        own_rows[q][1] = pl.ds(pl.multiple_of(co[first] * high + co[second] * step, step), step)
    scatter_a = [along(axes[q][0]) for q in range(3)]

    def pair_copy(t, i):
        ref = (s.g3, s.g2, s.g1)[i].at[t, 1 - t]
        index = grad_pair.base + 3 * t + i
        return pltpu.make_async_remote_copy(
            src_ref=ref, dst_ref=ref, send_sem=s.send_sem.at[index], recv_sem=s.recv_sem.at[index],
            device_id=(grad_pair.peers[0][2],), device_id_type=MESH)

    grad_pair = Exchange([(i, None, at_peer(AK, 1)) for i in range(6)])

    def hand_grads(t):
        @pl.when(k != t)
        def _():
            for i in range(3):
                pair_copy(t, i).start()

    def weight_grads(t):
        @pl.when(k == t)
        def _():
            def rows(ref, depth):
                return jnp.concatenate([ref[t, i] for i in range(nk)], axis=1)

            pair_copy(t, 0).wait_recv()
            third = mm(rows(s.h2t, WIDE), s.g3[t].reshape(nk * ROWS, EMB))
            for i in range(3):
                s.dw[2, 1, :, i * EMB:(i + 1) * EMB] = third[i * ROWS:(i + 1) * ROWS]
            pair_copy(t, 1).wait_recv()
            second = mm(rows(s.h1t, WIDE), s.g2[t].reshape(nk * ROWS, WIDE))
            s.dw[1, 0] = second[:ROWS]
            s.dw[1, 1] = second[ROWS:2 * ROWS]
            s.dw[2, 0] = second[2 * ROWS:]
            start_scatter(2)
            start_scatter(1)
            pair_copy(t, 2).wait_recv()
            first = mm(rows(s.xt, IN_WIDTH), s.g1[t].reshape(nk * ROWS, WIDE))
            s.dw[0, 0] = first[:ROWS]
            s.dw[0, 1] = first[ROWS:]
            start_scatter(0)

    def scatter_copy(q, i):
        high = ROWS // size[axes[q][0]]
        r, dest, dev = scatter_a[q].peers[i]
        index = scatter_a[q].base + i
        return pltpu.make_async_remote_copy(
            src_ref=s.dw.at[q, :, pl.ds(pl.multiple_of(dest * high, high), high)], dst_ref=s.ra[q].at[r - 1],
            send_sem=s.send_sem.at[index], recv_sem=s.recv_sem.at[index],
            device_id=(dev,), device_id_type=MESH)

    def start_scatter(q):
        for i in range(len(scatter_a[q].peers)):
            scatter_copy(q, i).start()

    grad_user = summed(0, du_x).T
    backward(0, grad_user)
    hand_grads(0)
    saved.recv()
    weight_grads(0)
    drain(middle)
    grad_item = summed(1, dv_x)
    backward(1, grad_item)
    hand_grads(1)
    weight_grads(1)
    order_q = (2, 1, 0)
    scatter_b = {}
    for q in order_q:
        for i in range(len(scatter_a[q].peers)):
            scatter_copy(q, i).wait_recv()
        first, second, _ = axes[q]
        value = s.dw[q, :, own_rows[q][0]]
        for r in range(size[first] - 1):
            value = value + s.ra[q][r]
        s.sa[q][...] = value
        step = ROWS // size[first] // size[second]
        scatter_b[q] = along(second).send(
            lambda r, d, q=q, step=step: s.sa[q].at[:, pl.ds(pl.multiple_of(d * step, step), step)],
            lambda r, d, q=q: s.rb[q].at[r - 1])
    for q in order_q:
        for i in range(len(scatter_a[q].peers)):
            scatter_copy(q, i).wait_send()
    for t in range(2):
        @pl.when(k != t)
        def _():
            for i in range(3):
                pair_copy(t, i).wait_send()
    second_end = len(started)
    exchange_c = {}
    for q in order_q:
        scatter_b[q].recv()
        first, second, third = axes[q]
        step = ROWS // size[first] // size[second]
        value = s.sa[q][:, pl.ds(pl.multiple_of(co[second] * step, step), step)]
        for r in range(size[second] - 1):
            value = value + s.rb[q][r]
        s.cx[q][co[third]] = value
        exchange_c[q] = share(third, s.cx[q].at[co[third]])
    drain(second_end)
    third_end = len(started)
    gather_b = {}
    for q in order_q:
        exchange_c[q].recv()
        value = s.cx[q][0]
        for r in range(1, size[axes[q][2]]):
            value = value + s.cx[q][r]
        out_ref[k, q, :, own_rows[q][1]] = value
        gather_b[q] = share(axes[q][1], out_ref.at[k, q, :, own_rows[q][1]])
    drain(third_end)
    loss_x.recv()
    loss_total = jnp.zeros((8, ROWS), F32)
    for ik in range(nk):
        for ix in range(nx):
            loss_total = loss_total + s.lx[ik, ix]
    loss_ref[...] = loss_total
    fourth_end = len(started)
    gather_a = {}
    handed = []
    for q in order_q:
        gather_b[q].recv()
        gather_a[q] = share(axes[q][0], out_ref.at[k, q, :, own_rows[q][0]])
    for q in order_q:
        handed.append(share(AK, out_ref.at[k, q, :, own_rows[q][0]]))
    drain(fourth_end)
    for i in range(max(size) - 1):
        for q in order_q:
            first = axes[q][0]
            high = ROWS // size[first]
            r = gather_a[q].peers[i][0]
            gather_a[q].copies[i].wait_recv()
            source = lax.rem(co[first] - r + size[first], size[first])
            handed.append(share(AK, out_ref.at[k, q, :, pl.ds(pl.multiple_of(source * high, high), high)]))
    for exchange in handed:
        exchange.recv()
    drain(len(started))


def finish_kernel(batch, res_ref, loss_in, loss_ref, *outs):
    loss_ref[...] = jnp.sum(loss_in[0:1], axis=1, keepdims=True) / batch
    for t in range(2):
        one, two, three = outs[3 * t:3 * t + 3]
        for i in range(2):
            one[i * ROWS:(i + 1) * ROWS] = res_ref[t, 0, i]
        for i in range(3):
            two[i * ROWS:(i + 1) * ROWS] = res_ref[t, 1 + i // 2, i % 2]
            three[i * ROWS:(i + 1) * ROWS] = res_ref[t, 2, 1, :, i * EMB:(i + 1) * EMB]


def solution(mesh):
    devices = mesh.shape['dp']
    grid = GRIDS[devices]
    scratch, tree = jax.tree.flatten(scratch_table(*grid))
    vmem = pl.BlockSpec(memory_space=pltpu.VMEM)
    hbm = pl.BlockSpec(memory_space=pltpu.HBM)

    def device_step(user_x, item_x, item_id, log_q, user_w1, user_w2, user_w3, item_w1, item_w2, item_w3):
        operands = (user_x, item_x, log_q.reshape(1, ROWS), item_id.reshape(1, ROWS),
                    user_w1, user_w2, user_w3, item_w1, item_w2, item_w3)
        res, loss_rows = pl.pallas_call(
            functools.partial(step_kernel, grid, tree),
            out_shape=(jax.ShapeDtypeStruct((2, 3, 2, ROWS, WIDE), F32), jax.ShapeDtypeStruct((8, ROWS), F32)),
            in_specs=[hbm] * 10,
            out_specs=(vmem, vmem),
            scratch_shapes=scratch,
            compiler_params=pltpu.CompilerParams(collective_id=0, has_side_effects=True, vmem_limit_bytes=40 * 1024 * 1024),
            name='train_step',
        )(*[pltpu.with_memory_space_constraint(value, pltpu.HBM) for value in operands])
        shapes = [(IN_WIDTH, WIDE), (WIDE, WIDE), (WIDE, EMB)] * 2
        outs = pl.pallas_call(
            functools.partial(finish_kernel, float(devices * ROWS)),
            out_shape=[jax.ShapeDtypeStruct((1, 1), F32)] + [jax.ShapeDtypeStruct(shape, F32) for shape in shapes],
            in_specs=[vmem, vmem],
            out_specs=[vmem] * 7,
            compiler_params=pltpu.CompilerParams(vmem_limit_bytes=12 * 1024 * 1024),
            name='finish',
        )(res, loss_rows)
        return (outs[0].reshape(()),) + tuple(outs[1:])

    rows, vec, whole = P('dp', None), P('dp'), P()
    return jax.shard_map(device_step, mesh=mesh, in_specs=(rows, rows, vec, vec) + (whole,) * 6,
                         out_specs=(whole,) * 7, check_vma=False)
```

```python
import functools

import jax
import jax.numpy as jnp
from jax import lax
from jax.experimental import pallas as pl
from jax.experimental.pallas import tpu as pltpu
from jax.sharding import PartitionSpec as P

MESH = pl.DeviceIdType.MESH
F32 = jnp.float32
BF16 = jnp.bfloat16
INV_TEMP = 1.0 / 0.05
NORM_EPS = 1e-6
ROWS = 128
EMB = 128
WIDE = 384
IN_WIDTH = 256
NEG = -3.0e38
GRIDS = {128: (4, 4, 4, 2), 16: (2, 2, 2, 2)}
AZ, AY, AX, AK = range(4)
C00 = (((0,), (0,)), ((), ()))
C11 = (((1,), (1,)), ((), ()))
C10 = (((1,), (0,)), ((), ()))
N_REMOTE = 208


def mm(a, b, dims=C10):
    return lax.dot_general(a, b, dims, preferred_element_type=F32)


def scratch_table(nz, ny, nx, nk):
    n_plane, n_small = nz * ny, nk * nx
    n_tile, tile_rows = nz + ny, ny * ROWS // 2
    n_query = n_small * ROWS
    n_wide = n_plane * ROWS
    longest = max(n_wide, n_query)
    turns = ((nx, ny, nz), (ny, nz, nx), (nz, nx, ny))

    def vm(dtype, *shape):
        return pltpu.VMEM(shape, dtype)

    def two(dtype, *shape):
        return [vm(dtype, *shape) for _ in range(2)]

    def each(shape_of):
        return [vm(F32, *shape_of(*turn), WIDE) for turn in turns]

    return dict(
        wh=[[vm(BF16, IN_WIDTH, WIDE), vm(BF16, WIDE, WIDE), vm(BF16, WIDE, EMB)] for _ in range(2)],
        xf=two(F32, ROWS, IN_WIDTH),
        wf=[[vm(F32, IN_WIDTH, WIDE), vm(F32, WIDE, WIDE), vm(F32, WIDE, EMB)] for _ in range(2)],
        lq=vm(F32, 1, ROWS),
        ids=vm(jnp.int32, 1, ROWS),
        h1=two(BF16, ROWS, WIDE),
        h2=two(BF16, ROWS, WIDE),
        xt=vm(BF16, 2, nk, IN_WIDTH, ROWS),
        h1t=vm(BF16, 2, nk, WIDE, ROWS),
        h2t=vm(BF16, 2, nk, WIDE, ROWS),
        g1=vm(BF16, 2, nk, ROWS, WIDE),
        g2=vm(BF16, 2, nk, ROWS, WIDE),
        g3=vm(BF16, 2, nk, ROWS, EMB),
        unit=two(F32, ROWS, EMB),
        inv=two(F32, ROWS, EMB),
        plane=two(BF16, nz, ny, ROWS, EMB),
        small=two(BF16, nk, nx, ROWS, EMB),
        parts=two(F32, n_small, ROWS, EMB),
        from_core=two(F32, nx, ROWS, EMB),
        core_sum=two(F32, nx, ROWS, EMB),
        from_x=two(F32, nx - 1, ROWS, EMB),
        dw=vm(F32, 3, 2, ROWS, WIDE),
        ra=each(lambda a, b, c: (a - 1, 2, ROWS // a)),
        sa=each(lambda a, b, c: (2, ROWS // a)),
        rb=each(lambda a, b, c: (b - 1, 2, ROWS // a // b)),
        cx=each(lambda a, b, c: (c, 2, ROWS // a // b)),
        meta_plane=vm(F32, nz, ny, 8, ROWS),
        meta_small=vm(F32, nk, nx, 8, ROWS),
        lqc_plane=vm(F32, nz, ny, ROWS, ROWS),
        idc_plane=vm(jnp.int32, nz, ny, ROWS, ROWS),
        lqc_small=vm(F32, n_small, ROWS, ROWS),
        idc_small=vm(jnp.int32, n_small, ROWS, ROWS),
        idr_plane=vm(jnp.int32, 1, n_wide),
        idr_small=vm(jnp.int32, 1, n_query),
        probs=vm(F32, n_tile, tile_rows, n_query),
        tile_max=vm(F32, n_tile, 1, n_query),
        tile_sum=vm(F32, n_tile, 1, n_query),
        factor=vm(F32, n_tile, 1, n_query),
        stats=vm(F32, nk, nx, 2 * n_small, ROWS),
        stat_all=vm(F32, 2 * n_small, ROWS),
        plane_t=vm(BF16, EMB, n_wide),
        user_t=vm(BF16, EMB, n_wide),
        item_tile=vm(BF16, 256, n_wide),
        grad_tile=vm(BF16, n_wide, 256),
        scores=vm(F32, n_small // 2, 256, n_wide),
        chunk_max=vm(F32, n_small // 2, 1, n_wide),
        row_max=vm(F32, 1, longest),
        row_inv=vm(F32, 1, longest),
        ml=vm(F32, nz, ny, 8, ROWS),
        lx=vm(F32, nk, nx, 8, ROWS),
        own_diag=vm(BF16, ROWS, ROWS),
        pos=vm(F32, 1, ROWS),
        send_sem=pltpu.SemaphoreType.DMA((N_REMOTE,)),
        recv_sem=pltpu.SemaphoreType.DMA((N_REMOTE,)),
        load_sem=pltpu.SemaphoreType.DMA((10,)),
    )


class Space:
    def __init__(self, entries):
        self.__dict__.update(entries)


def step_kernel(grid, tree, *refs):
    nz, ny, nx, nk = grid
    n_plane, n_small = nz * ny, nk * nx
    n_tile, tile_rows = nz + ny, ny * ROWS // 2
    n_chunk = n_small // 2
    n_query = n_small * ROWS
    n_wide = n_plane * ROWS
    batch = float(nz * ny * nx * nk * ROWS)
    x_in, lq_in, id_in = refs[0:2], refs[2], refs[3]
    w_in = (refs[4:7], refs[7:10])
    out_ref, loss_ref = refs[10:12]
    s = Space(jax.tree.unflatten(tree, refs[12:]))

    me = lax.axis_index('dp')
    size = grid
    stride = (ny * nx * nk, nx * nk, nk, 1)
    co = tuple(lax.rem(me // stride[ax], size[ax]) for ax in range(4))
    z, y, x, k = co

    def wrap(ax, r):
        return lax.rem(co[ax] + r, size[ax])

    def at_peer(ax, r):
        return me + (wrap(ax, r) - co[ax]) * stride[ax]

    def order(n):
        return sorted(range(1, n), key=lambda r: min(r, n - r))

    used = [0]
    started = []
    drained = [0]

    class Exchange:
        def __init__(self, peers):
            self.peers = peers
            self.base = used[0]
            used[0] += len(peers)
            self.copies = {}

        def post(self, index, src, dst):
            copy = pltpu.make_async_remote_copy(
                src_ref=src, dst_ref=dst,
                send_sem=s.send_sem.at[self.base + index], recv_sem=s.recv_sem.at[self.base + index],
                device_id=(self.peers[index][2],), device_id_type=MESH)
            copy.start()
            self.copies[index] = copy
            started.append(copy)

        def send(self, src, dst):
            for i, (r, dest, dev) in enumerate(self.peers):
                self.post(i, src(r, dest), dst(r, dest))
            return self

        def recv(self):
            for copy in self.copies.values():
                copy.wait_recv()

        def one(self, index, view):
            return pltpu.make_async_remote_copy(
                src_ref=view, dst_ref=view,
                send_sem=s.send_sem.at[self.base + index], recv_sem=s.recv_sem.at[self.base + index],
                device_id=(self.peers[0][2],), device_id_type=MESH)

    def along(ax):
        return Exchange([(r, wrap(ax, r), at_peer(ax, r)) for r in order(size[ax])])

    def share(ax, ref):
        return along(ax).send(lambda r, d: ref, lambda r, d: ref)

    def small_group():
        peers = []
        for rk in range(nk):
            for rx in [0] + order(nx):
                if rk or rx:
                    dev = me + (wrap(AK, rk) - k) + (wrap(AX, rx) - x) * nk
                    peers.append((len(peers), None, dev))
        return Exchange(peers)

    def plane_group():
        peers = []
        for rz in [0] + order(nz):
            for ry in [0] + order(ny):
                if rz or ry:
                    peers.append((len(peers), None, me + (wrap(AZ, rz) - z) * stride[AZ] + (wrap(AY, ry) - y) * stride[AY]))
        return Exchange(peers)

    def drain(upto):
        while drained[0] < upto:
            started[drained[0]].wait_send()
            drained[0] += 1

    loads = []

    def load(src, dst):
        copy = pltpu.make_async_copy(src, dst, s.load_sem.at[len(loads)])
        copy.start()
        loads.append(copy)
        return copy

    load_x, load_w = {}, {}
    for t in (1, 0):
        load_x[t] = load(x_in[t], s.xf[t])
        load_w[t] = [load(w_in[t][i], s.wf[t][i]) for i in range(3)]
        if t:
            load_meta = load(lq_in, s.lq), load(id_in, s.ids)

    barrier = pltpu.get_barrier_semaphore()
    greet = [at_peer(ax, r) for ax in (AZ, AY, AX, AK) for r in range(1, size[ax])]
    greet += [me + (wrap(AK, rk) - k) + (wrap(AX, rx) - x) * nk for rk in range(1, nk) for rx in range(1, nx)]
    greet += [me + (wrap(AZ, rz) - z) * stride[AZ] + (wrap(AY, ry) - y) * stride[AY] for rz in range(1, nz) for ry in range(1, ny)]
    for dev in greet:
        pl.semaphore_signal(barrier, inc=1, device_id=(dev,), device_id_type=MESH)

    def forward(t):
        load_x[t].wait()
        xb = s.xf[t][...].astype(BF16)
        for i in range(3):
            load_w[t][i].wait()
            s.wh[t][i][...] = s.wf[t][i][...].astype(BF16)
        act = jnp.maximum(mm(xb, s.wh[t][0][...]), 0.0).astype(BF16)
        s.h1[t][...] = act
        act = jnp.maximum(mm(act, s.wh[t][1][...]), 0.0).astype(BF16)
        s.h2[t][...] = act
        raw = mm(act, s.wh[t][2][...])
        inv = lax.rsqrt(jnp.sum(raw * raw, axis=1, keepdims=True) + NORM_EPS)
        unit = raw * inv
        s.unit[t][...] = unit
        s.inv[t][...] = jnp.broadcast_to(inv, (ROWS, EMB))
        half = unit.astype(BF16)
        s.plane[t][z, y] = half
        s.small[t][k, x] = half

    half_rows = ROWS // 2
    top, low = pl.ds(0, half_rows), pl.ds(half_rows, half_rows)

    def plane_first(t):
        ref = s.plane[t]
        return share(AY, ref.at[z, y, top]), share(AZ, ref.at[z, y, low])

    def plane_second(t, first):
        ref = s.plane[t]
        first[0].recv()
        a = share(AZ, ref.at[z, :, top])
        first[1].recv()
        b = share(AY, ref.at[:, y, low])
        return a, b

    forward(1)
    for copy in load_meta:
        copy.wait()
    ids = s.ids[...]
    zero_row = jnp.zeros((1, ROWS), F32)
    meta = jnp.concatenate([s.lq[...], lax.shift_right_logical(ids, 16).astype(F32),
                            lax.bitwise_and(ids, 65535).astype(F32)] + [zero_row] * 5, axis=0)
    s.meta_plane[z, y] = meta
    s.meta_small[k, x] = meta
    pl.semaphore_wait(barrier, len(greet))
    v_first = plane_first(1)
    meta_own = s.meta_plane.at[z, y, pl.ds(0, 3)]
    meta_wide = plane_group().send(lambda r, d: meta_own, lambda r, d: meta_own)
    meta_mine = s.meta_small.at[k, x, pl.ds(0, 3)]
    meta_near = small_group().send(lambda r, d: meta_mine, lambda r, d: meta_mine)
    v_small = share(AX, s.small[1].at[k, x])
    forward(0)
    u_small = share(AX, s.small[0].at[k, x])
    u_first = plane_first(0)
    v_second = plane_second(1, v_first)
    u_small.recv()
    u_small_k = share(AK, s.small[0].at[k])
    u_second = plane_second(0, u_first)
    v_small.recv()
    v_small_k = share(AK, s.small[1].at[k])

    def columns(ref, lq_out, id_out, id_row, count, nested):
        flat = ref[...].reshape(count * 8, ROWS)
        if count * 8 < ROWS:
            flat = jnp.concatenate([flat, jnp.zeros((ROWS - count * 8, ROWS), F32)], axis=0)
        turned = flat.T
        for i in range(count):
            lq_out[divmod(i, nested) if nested else i] = jnp.broadcast_to(turned[:, 8 * i:8 * i + 1], (ROWS, ROWS))
            hi = turned[:, 8 * i + 1:8 * i + 2].astype(jnp.int32)
            lo = turned[:, 8 * i + 2:8 * i + 3].astype(jnp.int32)
            id_out[divmod(i, nested) if nested else i] = jnp.broadcast_to(hi * 65536 + lo, (ROWS, ROWS))
            row_hi = flat[8 * i + 1:8 * i + 2].astype(jnp.int32)
            row_lo = flat[8 * i + 2:8 * i + 3].astype(jnp.int32)
            id_row[:, i * ROWS:(i + 1) * ROWS] = row_hi * 65536 + row_lo

    meta_near.recv()
    columns(s.meta_small, s.lqc_small, s.idc_small, s.idr_small, n_small, 0)
    meta_wide.recv()
    columns(s.meta_plane, s.lqc_plane, s.idc_plane, s.idr_plane, n_plane, ny)

    def transposed(value):
        return value.astype(F32).T.astype(BF16)

    for t in (0, 1):
        s.xt[t, k] = s.xf[t][...].T.astype(BF16)
        s.h1t[t, k] = transposed(s.h1[t][...])
        s.h2t[t, k] = transposed(s.h2[t][...])
    saved = Exchange([(i, None, at_peer(AK, 1)) for i in range(3)])
    for i, ref in enumerate((s.xt, s.h1t, s.h2t)):
        saved.post(i, ref.at[1 - k, k], ref.at[1 - k, k])
    saved_end = len(started)

    v_own = s.small[1][k, x]
    u_own = s.small[0][k, x]
    eye = (lax.broadcasted_iota(jnp.int32, (ROWS, ROWS), 0) == lax.broadcasted_iota(jnp.int32, (ROWS, ROWS), 1))
    own_scores = mm(v_own, u_own, C11) * INV_TEMP - s.lqc_small[k * nx + x]
    s.pos[...] = jnp.sum(jnp.where(eye, own_scores, 0.0), axis=0, keepdims=True)

    u_small_k.recv()

    def twice(value):
        return jnp.concatenate([value, value], axis=1)

    def score_tile(slot, items, lq_part, id_part):
        s.plane_t[:, pl.ds(pl.multiple_of(slot * tile_rows, tile_rows), tile_rows)] = transposed(items)
        lq_wide = twice(lq_part.reshape(tile_rows, ROWS))
        id_wide = twice(id_part.reshape(tile_rows, ROWS))
        for n in range(n_chunk):
            lanes = slice(n * 256, (n + 1) * 256)
            queries = s.small[0][2 * n // nx, pl.ds(2 * n % nx, 2)].reshape(256, EMB)
            score = mm(items, queries, C11) * INV_TEMP - lq_wide
            score = jnp.where(id_wide == s.idr_small[:, lanes], -jnp.inf, score)
            peak = jnp.maximum(jnp.max(score, axis=0, keepdims=True), NEG)
            prob = jnp.exp(score - peak)
            s.probs[slot, :, lanes] = prob
            s.tile_max[slot, :, lanes] = peak
            s.tile_sum[slot, :, lanes] = jnp.sum(prob, axis=0, keepdims=True)

    def score_step(index, carry):
        turn = jnp.where(index == 2, 3, jnp.where(index == 3, 2, index))
        ref = s.plane[1]

        @pl.when(index > 0)
        def _():
            for part, view in zip(v_second, (ref.at[z, :, top], ref.at[:, y, low])):
                part.one(index - 1, view).wait_recv()

        iz = lax.rem(z - turn + nz, nz)
        iy = lax.rem(y - turn + ny, ny)
        score_tile(2 * index, ref[iz, :, top].reshape(tile_rows, EMB), s.lqc_plane[iz, :, top], s.idc_plane[iz, :, top])
        score_tile(2 * index + 1, ref[:, iy, low].reshape(tile_rows, EMB), s.lqc_plane[:, iy, low], s.idc_plane[:, iy, low])
        return carry

    lax.fori_loop(0, nz, score_step, 0)

    tile_max = s.tile_max[...]
    part_max = jnp.max(tile_max, axis=0)
    part_sum = jnp.sum(s.tile_sum[...] * jnp.exp(tile_max - part_max[None]), axis=0)
    for i in range(n_small):
        s.stats[k, x, i:i + 1] = part_max[:, i * ROWS:(i + 1) * ROWS]
        s.stats[k, x, n_small + i:n_small + i + 1] = part_sum[:, i * ROWS:(i + 1) * ROWS]
    own_block = k * nx + x
    pos = s.pos[...]
    old_max = s.stats[k, x, pl.ds(own_block, 1)]
    new_max = jnp.maximum(old_max, pos)
    s.stats[k, x, pl.ds(own_block, 1)] = new_max
    s.stats[k, x, pl.ds(n_small + own_block, 1)] = (
        s.stats[k, x, pl.ds(n_small + own_block, 1)] * jnp.exp(old_max - new_max) + jnp.exp(pos - new_max))
    stats_ref = s.stats.at[k, x]
    stats = small_group().send(lambda r, d: stats_ref, lambda r, d: stats_ref)

    v_small_k.recv()
    for part in u_second:
        part.recv()

    stages = ((2, 1), (3, 0)) if nx == 4 else ((1, 0),)

    n_wide_tile = n_wide // 256

    def wide_tile(chunk, carry):
        side = jnp.where(lax.rem(chunk, 2) == 0, 1 - k, k)
        spots = []
        for turns in zip(*stages):
            spots.append(lax.rem(x + jnp.where(chunk // 2 == 0, turns[0], turns[-1]), nx))
        items = jnp.concatenate([s.small[1][side, spot] for spot in spots], axis=0)
        lq_wide = twice(jnp.concatenate([s.lqc_small[side * nx + spot] for spot in spots], axis=0))
        id_wide = twice(jnp.concatenate([s.idc_small[side * nx + spot] for spot in spots], axis=0))
        for n in range(n_wide_tile):
            lanes = slice(n * 256, (n + 1) * 256)
            queries = s.plane[0][2 * n // ny, pl.ds(2 * n % ny, 2)].reshape(256, EMB)
            score = mm(items, queries, C11) * INV_TEMP - lq_wide
            score = jnp.where(id_wide == s.idr_plane[:, lanes], -jnp.inf, score)
            peak = jnp.maximum(jnp.max(score, axis=0, keepdims=True), NEG)
            s.scores[chunk, :, lanes] = jnp.exp(score - peak)
            s.chunk_max[chunk, :, lanes] = peak
        return carry

    for iz in range(nz):
        for iy in range(ny):
            i = iz * ny + iy
            s.user_t[:, i * ROWS:(i + 1) * ROWS] = transposed(s.plane[0][iz, iy])
    lax.fori_loop(0, 3 * n_chunk // 4, wide_tile, 0)

    stats.recv()
    every = s.stats[...].reshape(n_small, 2 * n_small, ROWS)
    all_max = jnp.max(every[:, :n_small], axis=0)
    all_sum = jnp.zeros_like(all_max)
    for i in range(n_small):
        all_sum = all_sum + every[i, n_small:] * jnp.exp(every[i, :n_small] - all_max)
    all_inv = 1.0 / (all_sum * batch)
    s.stat_all[:n_small] = all_max
    s.stat_all[n_small:] = all_sum
    for i in range(n_small):
        s.row_max[:, i * ROWS:(i + 1) * ROWS] = all_max[i:i + 1]
        s.row_inv[:, i * ROWS:(i + 1) * ROWS] = all_inv[i:i + 1]
    own_max = s.stat_all[pl.ds(own_block, 1)]
    own_sum = s.stat_all[pl.ds(n_small + own_block, 1)]
    s.ml[z, y] = jnp.concatenate([own_max, own_sum, pos] + [zero_row] * 5, axis=0)
    ml_ref = s.ml.at[z, y, pl.ds(0, 3)]
    ml_plane = plane_group().send(lambda r, d: ml_ref, lambda r, d: ml_ref)
    own_grad = (jnp.exp(pos - own_max) / own_sum - 1.0) / batch
    s.own_diag[...] = jnp.where(eye, jnp.broadcast_to(own_grad, (ROWS, ROWS)), 0.0).astype(BF16)

    s.factor[...] = (jnp.exp(tile_max - s.row_max[:, :n_query][None]) * s.row_inv[:, :n_query][None])

    def user_chunk(index, carry):
        chunk = lax.rem((1 - k) * (n_chunk // 2) + index, n_chunk)
        lanes = pl.ds(pl.multiple_of(chunk * 256, 256), 256)
        for tile in range(n_tile):
            s.grad_tile[tile * tile_rows:(tile + 1) * tile_rows] = (
                s.probs[tile, :, lanes] * s.factor[tile, :, lanes]).astype(BF16)
        turned = mm(s.plane_t[...], s.grad_tile[...])
        s.parts[0][2 * chunk] = turned[:, :ROWS]
        s.parts[0][2 * chunk + 1] = turned[:, ROWS:]
        return carry

    def to_partner(t):
        ref = s.parts[t]
        into = s.from_core[t]
        return along(AK).send(lambda r, d: ref.at[pl.ds((1 - k) * nx, nx)], lambda r, d: into)

    def to_x(t, exchange):
        exchange.recv()
        for i in range(nx):
            s.core_sum[t][i] = s.parts[t][k * nx + i] + s.from_core[t][i]
        return along(AX).send(lambda r, d: s.core_sum[t].at[d], lambda r, d: s.from_x[t].at[r - 1])

    def summed(t, exchange):
        exchange.recv()
        total = s.core_sum[t][x]
        for r in range(1, nx):
            total = total + s.from_x[t][r - 1]
        return total * INV_TEMP

    lax.fori_loop(0, n_chunk // 2, user_chunk, 0)
    du_core = to_partner(0)
    lax.fori_loop(n_chunk // 2, n_chunk, user_chunk, 0)
    s.parts[0][own_block] = s.parts[0][own_block] + mm(v_own, s.own_diag[...], C00)
    du_x = to_x(0, du_core)
    drain(saved_end)
    lax.fori_loop(3 * n_chunk // 4, n_chunk, wide_tile, 0)
    ml_plane.recv()
    loss_row = jnp.zeros((1, ROWS), F32)
    for iz in range(nz):
        for iy in range(ny):
            i = iz * ny + iy
            row = s.ml[iz, iy]
            s.row_max[:, i * ROWS:(i + 1) * ROWS] = row[0:1]
            s.row_inv[:, i * ROWS:(i + 1) * ROWS] = 1.0 / (row[1:2] * batch)
            loss_row = loss_row + ((row[0:1] - row[2:3]) + jnp.log(row[1:2]))
    s.lx[k, x] = jnp.broadcast_to(loss_row, (8, ROWS))
    lx_ref = s.lx.at[k, x]
    loss_x = small_group().send(lambda r, d: lx_ref, lambda r, d: lx_ref)

    def item_chunk(stage, side, own):
        chunk = 2 * stage + own
        for n in range(n_wide_tile):
            lanes = slice(n * 256, (n + 1) * 256)
            factor = jnp.exp(s.chunk_max[chunk, :, lanes] - s.row_max[:, lanes]) * s.row_inv[:, lanes]
            s.item_tile[:, lanes] = (s.scores[chunk, :, lanes] * factor).astype(BF16)
        total = mm(s.user_t[...], s.item_tile[...], C11)
        for i, r in enumerate(stages[stage]):
            s.parts[1][side * nx + wrap(AX, r)] = total[:, i * ROWS:(i + 1) * ROWS]

    dv_core = Exchange([(i, None, at_peer(AK, 1)) for i in range(nx)])
    dv_x = along(AX)
    for stage, turns in enumerate(stages):
        item_chunk(stage, 1 - k, 0)
        for i, r in enumerate(turns):
            spot = wrap(AX, r)
            dv_core.post(2 * stage + i, s.parts[1].at[(1 - k) * nx + spot], s.from_core[1].at[spot])
        item_chunk(stage, k, 1)
        if 0 in turns:
            s.parts[1][own_block] = s.parts[1][own_block] + mm(u_own, s.own_diag[...], C00)
        for i, r in enumerate(turns):
            spot = wrap(AX, r)
            dv_core.copies[2 * stage + i].wait_recv()
            s.core_sum[1][spot] = s.parts[1][k * nx + spot] + s.from_core[1][spot]
            if r:
                dv_x.post(order(nx).index(r), s.core_sum[1].at[spot], s.from_x[1].at[r - 1])
    middle = len(started)

    def backward(t, grad_unit):
        unit = s.unit[t][...]
        grad_raw = s.inv[t][...] * (grad_unit - unit * jnp.sum(unit * grad_unit, axis=1, keepdims=True))
        grad_three = grad_raw.astype(BF16)
        s.g3[t, k] = grad_three
        back = mm(grad_three, s.wh[t][2][...], C11)
        grad_two = jnp.where(s.h2[t][...] > 0, back, 0.0).astype(BF16)
        s.g2[t, k] = grad_two
        back = mm(grad_two, s.wh[t][1][...], C11)
        s.g1[t, k] = jnp.where(s.h1[t][...] > 0, back, 0.0).astype(BF16)

    axes = ((AX, AY, AZ), (AY, AZ, AX), (AZ, AX, AY))
    own_rows = [[None, None] for _ in axes]
    for q, (first, second, _) in enumerate(axes):
        high = ROWS // size[first]
        step = high // size[second]
        own_rows[q][0] = pl.ds(pl.multiple_of(co[first] * high, high), high)
        own_rows[q][1] = pl.ds(pl.multiple_of(co[first] * high + co[second] * step, step), step)
    scatter_a = [along(axes[q][0]) for q in range(3)]

    def pair_copy(t, i):
        ref = (s.g3, s.g2, s.g1)[i].at[t, 1 - t]
        index = grad_pair.base + 3 * t + i
        return pltpu.make_async_remote_copy(
            src_ref=ref, dst_ref=ref, send_sem=s.send_sem.at[index], recv_sem=s.recv_sem.at[index],
            device_id=(grad_pair.peers[0][2],), device_id_type=MESH)

    grad_pair = Exchange([(i, None, at_peer(AK, 1)) for i in range(6)])

    def hand_grads(t):
        @pl.when(k != t)
        def _():
            for i in range(3):
                pair_copy(t, i).start()

    def weight_grads(t):
        @pl.when(k == t)
        def _():
            def rows(ref, depth):
                return jnp.concatenate([ref[t, i] for i in range(nk)], axis=1)

            pair_copy(t, 0).wait_recv()
            third = mm(rows(s.h2t, WIDE), s.g3[t].reshape(nk * ROWS, EMB))
            for i in range(3):
                s.dw[2, 1, :, i * EMB:(i + 1) * EMB] = third[i * ROWS:(i + 1) * ROWS]
            pair_copy(t, 1).wait_recv()
            second = mm(rows(s.h1t, WIDE), s.g2[t].reshape(nk * ROWS, WIDE))
            s.dw[1, 0] = second[:ROWS]
            s.dw[1, 1] = second[ROWS:2 * ROWS]
            s.dw[2, 0] = second[2 * ROWS:]
            start_scatter(2)
            start_scatter(1)
            pair_copy(t, 2).wait_recv()
            first = mm(rows(s.xt, IN_WIDTH), s.g1[t].reshape(nk * ROWS, WIDE))
            s.dw[0, 0] = first[:ROWS]
            s.dw[0, 1] = first[ROWS:]
            start_scatter(0)

    def scatter_copy(q, i):
        high = ROWS // size[axes[q][0]]
        r, dest, dev = scatter_a[q].peers[i]
        index = scatter_a[q].base + i
        return pltpu.make_async_remote_copy(
            src_ref=s.dw.at[q, :, pl.ds(pl.multiple_of(dest * high, high), high)], dst_ref=s.ra[q].at[r - 1],
            send_sem=s.send_sem.at[index], recv_sem=s.recv_sem.at[index],
            device_id=(dev,), device_id_type=MESH)

    def start_scatter(q):
        for i in range(len(scatter_a[q].peers)):
            scatter_copy(q, i).start()

    grad_user = summed(0, du_x).T
    backward(0, grad_user)
    hand_grads(0)
    saved.recv()
    weight_grads(0)
    drain(middle)
    grad_item = summed(1, dv_x).T
    backward(1, grad_item)
    hand_grads(1)
    weight_grads(1)
    order_q = (2, 1, 0)
    scatter_b = {}
    for q in order_q:
        for i in range(len(scatter_a[q].peers)):
            scatter_copy(q, i).wait_recv()
        first, second, _ = axes[q]
        value = s.dw[q, :, own_rows[q][0]]
        for r in range(size[first] - 1):
            value = value + s.ra[q][r]
        s.sa[q][...] = value
        step = ROWS // size[first] // size[second]
        scatter_b[q] = along(second).send(
            lambda r, d, q=q, step=step: s.sa[q].at[:, pl.ds(pl.multiple_of(d * step, step), step)],
            lambda r, d, q=q: s.rb[q].at[r - 1])
    for q in order_q:
        for i in range(len(scatter_a[q].peers)):
            scatter_copy(q, i).wait_send()
    for t in range(2):
        @pl.when(k != t)
        def _():
            for i in range(3):
                pair_copy(t, i).wait_send()
    second_end = len(started)
    exchange_c = {}
    for q in order_q:
        scatter_b[q].recv()
        first, second, third = axes[q]
        step = ROWS // size[first] // size[second]
        value = s.sa[q][:, pl.ds(pl.multiple_of(co[second] * step, step), step)]
        for r in range(size[second] - 1):
            value = value + s.rb[q][r]
        s.cx[q][co[third]] = value
        exchange_c[q] = share(third, s.cx[q].at[co[third]])
    drain(second_end)
    third_end = len(started)
    gather_b = {}
    for q in order_q:
        exchange_c[q].recv()
        value = s.cx[q][0]
        for r in range(1, size[axes[q][2]]):
            value = value + s.cx[q][r]
        out_ref[k, q, :, own_rows[q][1]] = value
        gather_b[q] = share(axes[q][1], out_ref.at[k, q, :, own_rows[q][1]])
    drain(third_end)
    loss_x.recv()
    loss_total = jnp.zeros((8, ROWS), F32)
    for ik in range(nk):
        for ix in range(nx):
            loss_total = loss_total + s.lx[ik, ix]
    loss_ref[...] = loss_total
    fourth_end = len(started)
    gather_a = {}
    handed = []
    for q in order_q:
        gather_b[q].recv()
        gather_a[q] = share(axes[q][0], out_ref.at[k, q, :, own_rows[q][0]])
    for q in order_q:
        handed.append(share(AK, out_ref.at[k, q, :, own_rows[q][0]]))
    drain(fourth_end)
    for i in range(max(size) - 1):
        for q in order_q:
            first = axes[q][0]
            high = ROWS // size[first]
            r = gather_a[q].peers[i][0]
            gather_a[q].copies[i].wait_recv()
            source = lax.rem(co[first] - r + size[first], size[first])
            handed.append(share(AK, out_ref.at[k, q, :, pl.ds(pl.multiple_of(source * high, high), high)]))
    for exchange in handed:
        exchange.recv()
    drain(len(started))


def finish_kernel(batch, res_ref, loss_in, loss_ref, *outs):
    loss_ref[...] = jnp.sum(loss_in[0:1], axis=1, keepdims=True) / batch
    for t in range(2):
        one, two, three = outs[3 * t:3 * t + 3]
        for i in range(2):
            one[i * ROWS:(i + 1) * ROWS] = res_ref[t, 0, i]
        for i in range(3):
            two[i * ROWS:(i + 1) * ROWS] = res_ref[t, 1 + i // 2, i % 2]
            three[i * ROWS:(i + 1) * ROWS] = res_ref[t, 2, 1, :, i * EMB:(i + 1) * EMB]


def solution(mesh):
    devices = mesh.shape['dp']
    grid = GRIDS[devices]
    scratch, tree = jax.tree.flatten(scratch_table(*grid))
    vmem = pl.BlockSpec(memory_space=pltpu.VMEM)
    hbm = pl.BlockSpec(memory_space=pltpu.HBM)

    def device_step(user_x, item_x, item_id, log_q, user_w1, user_w2, user_w3, item_w1, item_w2, item_w3):
        operands = (user_x, item_x, log_q.reshape(1, ROWS), item_id.reshape(1, ROWS),
                    user_w1, user_w2, user_w3, item_w1, item_w2, item_w3)
        res, loss_rows = pl.pallas_call(
            functools.partial(step_kernel, grid, tree),
            out_shape=(jax.ShapeDtypeStruct((2, 3, 2, ROWS, WIDE), F32), jax.ShapeDtypeStruct((8, ROWS), F32)),
            in_specs=[hbm] * 10,
            out_specs=(vmem, vmem),
            scratch_shapes=scratch,
            compiler_params=pltpu.CompilerParams(collective_id=0, has_side_effects=True, vmem_limit_bytes=40 * 1024 * 1024),
            name='train_step',
        )(*[pltpu.with_memory_space_constraint(value, pltpu.HBM) for value in operands])
        shapes = [(IN_WIDTH, WIDE), (WIDE, WIDE), (WIDE, EMB)] * 2
        outs = pl.pallas_call(
            functools.partial(finish_kernel, float(devices * ROWS)),
            out_shape=[jax.ShapeDtypeStruct((1, 1), F32)] + [jax.ShapeDtypeStruct(shape, F32) for shape in shapes],
            in_specs=[vmem, vmem],
            out_specs=[vmem] * 7,
            compiler_params=pltpu.CompilerParams(vmem_limit_bytes=12 * 1024 * 1024),
            name='finish',
        )(res, loss_rows)
        return (outs[0].reshape(()),) + tuple(outs[1:])

    rows, vec, whole = P('dp', None), P('dp'), P()
    return jax.shard_map(device_step, mesh=mesh, in_specs=(rows, rows, vec, vec) + (whole,) * 6,
                         out_specs=(whole,) * 7, check_vma=False)
```
